128 devices in a mesh: lat: 8 (over z, x_hi), lon: 16 (over y, x_lo, core).
Axes of the slice: x: 4 (x_hi: 2, x_lo: 2; x = x_hi * 2 + x_lo), y: 4, z: 4, core: 2. Of those that a mesh axis runs over, the one named last changes fastest.
Arguments:
- fine_field: bfloat16 [128, 768, 128], P('lat', 'lon'), may hold values from -6 to 6
- w_enc: bfloat16 [3, 3, 128, 128], replicated, may hold values from -0.1875 to 0.1875
- w_down: bfloat16 [128, 512], replicated, may hold values from -0.5 to 0.5
- w_bot: bfloat16 [3, 3, 512, 512], replicated, may hold values from -0.09375 to 0.09375
- w_up: bfloat16 [512, 128], replicated, may hold values from -0.25 to 0.25
- w_dec: bfloat16 [3, 3, 128, 128], replicated, may hold values from -0.1875 to 0.1875
- out_grad: bfloat16 [128, 768, 128], P('lat', 'lon'), may hold values from -6 to 6
Outputs:
- block_out: bfloat16 [128, 768, 128], P('lat', 'lon')
- field_grad: bfloat16 [128, 768, 128], P('lat', 'lon')
- g_enc: float32 [3, 3, 128, 128], replicated
- g_down: float32 [128, 512], replicated
- g_bot: float32 [3, 3, 512, 512], replicated
- g_up: float32 [512, 128], replicated
- g_dec: float32 [3, 3, 128, 128], replicated
The draws below stay inside these ranges and needn't reach their ends.
All inputs are finite; a program needn't handle non-finite values.
Results may differ from the reference program's by a relative error of at most 0.015.
Values may be sent and summed in bfloat16 or wider, within the bound.
No kernel may reach another device: no remote copies, remote signals or barrier semaphores. Data moves between devices by JAX's collectives and lax.ppermute only.
A program may use at most 128 MiB of HBM per device.

```python
import jax
import jax.numpy as jnp
from jax import lax

C = 128
B = 512
POOL = 8
NH = 128
NW = 768


def block_levels(stream_key, shape, shards, low, high):
    def one(dim, shards_of):
        steps = jax.random.uniform(jax.random.fold_in(jax.random.fold_in(stream_key, 6), dim), (shards_of,), jnp.float32, low / len(shards), high / len(shards))
        return jnp.repeat(jnp.exp(steps), shape[dim] // shards_of).reshape((-1,) + (1,) * (len(shape) - dim - 1))

    gain = one(*shards[0])
    for cut in shards[1:]:
        gain = gain * one(*cut)
    return gain


def noise(key, dims, width, most, cuts=(), kind=jnp.bfloat16):
    array = jax.random.normal(key, dims, jnp.float32) * width
    if len(cuts) > 0:
        array = block_levels(key, dims, cuts, -0.22, 0.18) * array
    return jnp.clip(array, min=-most, max=most).astype(kind)


def setup_inputs(seed: int = 0) -> dict:
    arg_keys = jax.random.split(jax.random.key(seed), 8)
    fine_field = noise(arg_keys[0], (NH, NW, C), 1.0, 6.0, ((0, 8), (1, 16)))
    w_enc = noise(arg_keys[1], (3, 3, C, C), (9 * C) ** -0.5, 0.1875)
    w_down = noise(arg_keys[2], (C, B), C ** -0.5, 0.5)
    w_bot = noise(arg_keys[3], (3, 3, B, B), (9 * B) ** -0.5, 0.09375)
    w_up = noise(arg_keys[4], (B, C), B ** -0.5, 0.25)
    w_dec = noise(arg_keys[5], (3, 3, C, C), (9 * C) ** -0.5, 0.1875)
    out_grad = noise(arg_keys[6], (NH, NW, C), 1.0, 6.0, ((0, 8), (1, 16)))
    return dict(fine_field=fine_field, w_enc=w_enc, w_down=w_down, w_bot=w_bot, w_up=w_up, w_dec=w_dec, out_grad=out_grad)


def moved(field, down, across):
    height = field.shape[0]
    padded = jnp.pad(field, ((1, 1), (0, 0), (0, 0)))
    rolled = jnp.roll(padded, -across, axis=1)
    return rolled[1 + down:1 + down + height]

def conv_fwd(field, kernel):
    height, breadth, depth = field.shape
    total = jnp.zeros((height * breadth, kernel.shape[3]), jnp.float32)
    for tap_a in range(3):
        for tap_b in range(3):
            view = moved(field, tap_a - 1, tap_b - 1).reshape(-1, depth)
            total = total + jnp.dot(view, kernel[tap_a, tap_b], preferred_element_type=jnp.float32)
    return total.reshape(height, breadth, kernel.shape[3])

def conv_back(grad, kernel):
    height, breadth, depth = grad.shape
    total = jnp.zeros((height * breadth, kernel.shape[2]), jnp.float32)
    for tap_a in range(3):
        for tap_b in range(3):
            view = moved(grad, 1 - tap_a, 1 - tap_b).reshape(-1, depth)
            total = total + jnp.dot(view, kernel[tap_a, tap_b].T, preferred_element_type=jnp.float32)
    return total.reshape(height, breadth, kernel.shape[2])

def cross(left, right):
    return lax.dot_general(left.reshape(-1, left.shape[-1]), right.reshape(-1, right.shape[-1]), (((0,), (0,)), ((), ())), preferred_element_type=jnp.float32)

def kernel_grad(field, grad):
    rows_out = []
    for tap_a in range(3):
        row_list = []
        for tap_b in range(3):
            row_list.append(cross(moved(field, tap_a - 1, tap_b - 1), grad))
        rows_out.append(jnp.stack(row_list))
    return jnp.stack(rows_out)

def mapped(field, matrix):
    flat = jnp.dot(field.reshape(-1, field.shape[-1]), matrix, preferred_element_type=jnp.float32)
    return flat.reshape(field.shape[:-1] + (matrix.shape[1],))

def slope(value):
    sig = jax.nn.sigmoid(value)
    return sig * (1.0 + value * (1.0 - sig))

def block_total(field):
    height, breadth, depth = field.shape
    return field.astype(jnp.float32).reshape(height // POOL, POOL, breadth // POOL, POOL, depth).sum(axis=(1, 3))

def repeated(field):
    return jnp.repeat(jnp.repeat(field, POOL, axis=0), POOL, axis=1)

def reference(fine_field, w_enc, w_down, w_bot, w_up, w_dec, out_grad):
    act = conv_fwd(fine_field, w_enc)
    hid = jax.nn.silu(act).astype(jnp.bfloat16)
    pooled = (block_total(hid) / (POOL * POOL)).astype(jnp.bfloat16)
    coarse = mapped(pooled, w_down).astype(jnp.bfloat16)
    zpre = conv_fwd(coarse, w_bot)
    zact = jax.nn.silu(zpre).astype(jnp.bfloat16)
    lifted = mapped(zact, w_up)
    merged = (hid.astype(jnp.float32) + repeated(lifted)).astype(jnp.bfloat16)
    block_out = conv_fwd(merged, w_dec).astype(jnp.bfloat16)
    dmerged = conv_back(out_grad, w_dec)
    g_dec = kernel_grad(merged, out_grad)
    dlift = block_total(dmerged).astype(jnp.bfloat16)
    g_up = cross(zact, dlift)
    dzpre = (mapped(dlift, w_up.T) * slope(zpre)).astype(jnp.bfloat16)
    g_bot = kernel_grad(coarse, dzpre)
    dcoarse = conv_back(dzpre, w_bot).astype(jnp.bfloat16)
    g_down = cross(pooled, dcoarse)
    dpool = mapped(dcoarse, w_down.T)
    dact = ((dmerged + repeated(dpool) / (POOL * POOL)) * slope(act)).astype(jnp.bfloat16)
    field_grad = conv_back(dact, w_enc).astype(jnp.bfloat16)
    g_enc = kernel_grad(fine_field, dact)
    return (block_out, field_grad, g_enc, g_down, g_bot, g_up, g_dec)
```

```python
import jax
import jax.numpy as jnp
from jax import lax
from jax.experimental import pallas as pl
from jax.experimental.pallas import tpu as pltpu
from jax.sharding import PartitionSpec as P

POOL = 8
AXES = ("lat", "lon")
ROWS, COLS, DEPTH = 16, 48, 128
WIDE = 512
STRIDE = 64
EXT = 21 * STRIDE
RIM = 19 * STRIDE
OWN = ROWS * STRIDE
CROW, CCOL = ROWS // POOL, COLS // POOL
NLAT, NLON = 8, 16
COUNT = NLAT * NLON
GROW, GCOL = NLAT * CROW, NLON * CCOL
CELLS = GROW * GCOL
PACK = 2 * CROW * CCOL
WIN = 16
F32 = jnp.float32
BF16 = jnp.bfloat16


def mm(left, right, contract=((1,), (0,))):
    return lax.dot_general(left, right, (contract, ((), ())), preferred_element_type=F32)


def side_by_side(flat):
    wide = flat.astype(F32)
    low = pltpu.roll(wide, 1, 0).astype(BF16)
    high = pltpu.roll(wide, flat.shape[0] - 1, 0).astype(BF16)
    return jnp.concatenate([low, flat.astype(BF16), high], axis=1)


def split_two(value):
    high = value.astype(BF16)
    return high, (value - high.astype(F32)).astype(BF16)


def rim_position(shape, dim):
    spot = lax.broadcasted_iota(jnp.int32, shape, dim)
    slot = spot & (STRIDE - 1)
    line = spot >> 6
    left = slot == STRIDE - 1
    row = jnp.where(left, line - 1, line - 2)
    col = jnp.where(left, -1, slot)
    return row, col


def row_live(row, lat):
    return jnp.logical_and(
        jnp.logical_or(row >= 0, lat > 0), jnp.logical_or(row < ROWS, lat < NLAT - 1)
    )


def first_kernel(
    pos, fine, grad, top, bot, strip, w_enc, w_dec_t,
    pack, hid_out, slope_out, dm_out, fine_cat, own_grad, field, grad_cat,
):
    lat = pos[0]
    for part, (tile, cat) in enumerate(((fine, fine_cat), (grad, grad_cat))):
        lanes = slice(part * DEPTH, (part + 1) * DEPTH)
        field[0:1, 0:COLS, :] = jnp.zeros((1, COLS, DEPTH), BF16)
        field[1:3, 0:COLS, :] = top[:, :, lanes]
        field[3:19, 0:COLS, :] = tile[...]
        field[19:21, 0:COLS, :] = bot[:, :, lanes]
        field[:, COLS:STRIDE, :] = strip[:, :, lanes]
        cat[...] = side_by_side(field[...].reshape(EXT, DEPTH))
    act = jnp.zeros((RIM, DEPTH), F32)
    dm = jnp.zeros((RIM, DEPTH), F32)
    for tap in range(3):
        act = act + mm(fine_cat[tap * STRIDE : tap * STRIDE + RIM, :], w_enc[tap])
        dm = dm + mm(grad_cat[tap * STRIDE : tap * STRIDE + RIM, :], w_dec_t[tap])
    row, _ = rim_position((RIM, 1), 0)
    live = row_live(row, lat)
    sig = jax.nn.sigmoid(act)
    hid = jnp.where(live, act * sig, 0.0).astype(BF16)
    slope_out[...] = jnp.where(live, sig * (1.0 + act * (1.0 - sig)), 0.0)
    hid_out[...] = hid
    dm_out[...] = dm
    half = PACK // 2
    prow, pcol = rim_position((PACK, RIM), 1)
    which = lax.broadcasted_iota(jnp.int32, (PACK, RIM), 0)
    inside = (prow >= 0) & (prow < ROWS) & (pcol >= 0) & (pcol < COLS)
    cell = jnp.where(inside, (prow >> 3) * CCOL + (pcol >> 3), -1)
    take_hid = (cell == which).astype(F32).astype(BF16)
    take_dm = (inside & (cell + half == which)).astype(F32).astype(BF16)
    dm_high, dm_low = split_two(dm)
    packed = mm(take_hid, hid) * (1.0 / (POOL * POOL)) + (mm(take_dm, dm_high) + mm(take_dm, dm_low))
    packed = packed.astype(BF16)
    for peer in range(COUNT):
        pack[peer] = packed
    slot = lax.broadcasted_iota(jnp.int32, (OWN, 1), 0) & (STRIDE - 1)
    center = grad_cat[3 * STRIDE : 3 * STRIDE + OWN, DEPTH : 2 * DEPTH]
    own_grad[...] = jnp.where(slot < COLS, center, jnp.zeros_like(center))


def weight_kernel(w_down, w_bot, out):
    out[0] = mm(w_down[...], w_bot[0]).astype(BF16)


def third(value):
    return (value * 43) >> 8


def source_of(row, col, shift):
    inside = (row >= 0) & (row < GROW)
    col = jnp.where(col < 0, col + GCOL, col)
    col = jnp.where(col >= GCOL, col - GCOL, col)
    group = third(col)
    device = (row >> 1) * NLON + group
    return jnp.where(inside, device * PACK + shift + (row & 1) * CCOL + (col - group * CCOL), -1)


def second_kernel(
    pos, every, w_eff, w_up, hid, slope, dm, fine_cat, own_grad, parts, merged_cat, dact_cat
):
    lat, lon = pos[0], pos[1]
    spot = lax.broadcasted_iota(jnp.int32, (8 * WIN, 1), 0)
    line, slot = spot >> 4, spot & (WIN - 1)
    src = source_of(CROW * lat + line - 3, CCOL * lon + slot - 3, 0)
    src = jnp.where(slot < CCOL + 6, src, -1)
    spot = lax.broadcasted_iota(jnp.int32, (6 * WIN, 1), 0)
    line, slot = spot >> 4, spot & (WIN - 1)
    dsrc = source_of(CROW * lat + line - 2, CCOL * lon + slot - 2, CROW * CCOL)
    dsrc = jnp.where(slot < CCOL + 4, dsrc, -1)
    spots = lax.broadcasted_iota(jnp.int32, (8 * WIN, COUNT * PACK), 1)
    pooled = mm((spots == src).astype(F32).astype(BF16), every[...])
    spots = lax.broadcasted_iota(jnp.int32, (6 * WIN, COUNT * PACK), 1)
    dlift = mm((spots == dsrc).astype(F32).astype(BF16), every[...]).astype(BF16)
    shifted = [pooled.astype(BF16)] + [
        pltpu.roll(pooled, 8 * WIN - step, 0).astype(BF16) for step in (1, 2)
    ]
    pooled_cat = jnp.concatenate(shifted, axis=1)
    zpre = jnp.zeros((6 * WIN, WIDE), F32)
    for tap in range(3):
        zpre = zpre + mm(
            pooled_cat[tap * WIN : tap * WIN + 6 * WIN], w_eff[tap * 384 : tap * 384 + 384, :]
        )
    sig = jax.nn.sigmoid(zpre)
    zact = (zpre * sig).astype(BF16)
    dz = mm(dlift, w_up[...], ((1,), (1,))) * (sig * (1.0 + zpre * (1.0 - sig)))
    dz = dz.astype(BF16).astype(F32)
    lifted = mm(zact, w_up[...])
    gap = jnp.zeros((WIN, WIDE), F32)
    padded = jnp.concatenate([gap, dz, gap], axis=0)
    dpool = jnp.zeros((6 * WIN, DEPTH), F32)
    for tap_b in range(3):
        turn = (1 - tap_b) % (8 * WIN)
        moved = (padded if turn == 0 else pltpu.roll(padded, turn, 0)).astype(BF16)
        for tap_a in range(3):
            spot = ((2 - tap_a) * 3 + (2 - tap_b)) * DEPTH
            dpool = dpool + mm(
                moved[tap_a * WIN : tap_a * WIN + 6 * WIN],
                w_eff[spot : spot + DEPTH, :],
                ((1,), (1,)),
            )
    dpool = dpool * (1.0 / (POOL * POOL))
    lift_high, lift_low = split_two(lifted)
    pool_high, pool_low = split_two(dpool)
    tail = jnp.zeros((2 * WIN, 2 * DEPTH), BF16)
    table = jnp.concatenate(
        [
            jnp.concatenate([lift_high, pool_high], axis=1),
            tail,
            jnp.concatenate([lift_low, pool_low], axis=1),
            tail,
        ],
        axis=0,
    )
    row, col = rim_position((RIM, 1), 0)
    home = (((row + POOL) >> 3) + 1) * WIN + ((col + POOL) >> 3) + 1
    home = jnp.where(col <= COLS, home, -1)
    cells = lax.broadcasted_iota(jnp.int32, (RIM, 256), 1) & 127
    spread = mm((cells == home).astype(F32).astype(BF16), table)
    live = row_live(row, lat)
    merged = jnp.where(live, hid[...].astype(F32) + spread[:, :DEPTH], 0.0)
    dact = (dm[...] + spread[:, DEPTH:]) * slope[...]
    merged_cat[...] = side_by_side(merged.astype(BF16))
    dact_cat[...] = side_by_side(dact.astype(BF16))
    slot = lax.broadcasted_iota(jnp.int32, (OWN, 1), 0) & (STRIDE - 1)
    center = dact_cat[2 * STRIDE : 2 * STRIDE + OWN, DEPTH : 2 * DEPTH]
    own_dact = jnp.where(slot < COLS, center, jnp.zeros_like(center))
    for tap in range(3):
        start = (tap + 1) * STRIDE
        parts[tap * 384 : tap * 384 + 384, :] = mm(
            merged_cat[start : start + OWN, :], own_grad[...], ((0,), (0,))
        ).astype(BF16)
        start = (tap + 2) * STRIDE
        parts[1152 + tap * 384 : 1152 + tap * 384 + 384, :] = mm(
            fine_cat[start : start + OWN, :], own_dact, ((0,), (0,))
        ).astype(BF16)
    parts[2304:, :] = jnp.zeros((COUNT * PACK - 2304, DEPTH), BF16)


def third_kernel(merged_cat, dact_cat, w_dec, w_enc_t, block_out, field_grad):
    out = jnp.zeros((OWN, DEPTH), F32)
    back = jnp.zeros((OWN, DEPTH), F32)
    for tap in range(3):
        start = (tap + 1) * STRIDE
        out = out + mm(merged_cat[start : start + OWN, :], w_dec[tap])
        back = back + mm(dact_cat[start : start + OWN, :], w_enc_t[tap])
    block_out[...] = out.astype(BF16).reshape(ROWS, STRIDE, DEPTH)[:, :COLS, :]
    field_grad[...] = back.astype(BF16).reshape(ROWS, STRIDE, DEPTH)[:, :COLS, :]


def coarse_kernel(
    every, w_eff, w_up, w_down, w_bot, g_bot, g_down, g_up, pooled_cat, dlift, zact, dz, table
):
    step = pl.program_id(0)
    line = 2 * GCOL

    @pl.when(step == 0)
    def _():
        block = NLON * PACK
        spot = lax.broadcasted_iota(jnp.int32, (4 * line, 1), 0)
        kind = (spot >= line).astype(jnp.int32) + (spot >= 2 * line).astype(jnp.int32)
        kind = kind + (spot >= 3 * line).astype(jnp.int32)
        within = spot - kind * line
        row = (within >= GCOL).astype(jnp.int32)
        col = within - row * GCOL
        col = jnp.where(kind < 3, col + kind - 1, col)
        shift = jnp.where(kind < 3, 0, CROW * CCOL)
        src = source_of(row, col, shift)
        spots = lax.broadcasted_iota(jnp.int32, (4 * line, block), 1)
        order = (spots == src).astype(F32).astype(BF16)
        edge = jnp.zeros((GCOL, 3 * DEPTH), BF16)
        pooled_cat[0:GCOL, :] = edge
        pooled_cat[(GROW + 1) * GCOL :, :] = edge
        for pair in range(NLAT // 2):
            both = jnp.concatenate(
                [every[(2 * pair + k) * block : (2 * pair + k + 1) * block, :] for k in (0, 1)],
                axis=1,
            )
            moved = mm(order, both).astype(BF16)
            for k in (0, 1):
                lat = 2 * pair + k
                lanes = slice(k * DEPTH, (k + 1) * DEPTH)
                at = GCOL + lat * line
                for b in range(3):
                    pooled_cat[at : at + line, b * DEPTH : (b + 1) * DEPTH] = moved[
                        b * line : (b + 1) * line, lanes
                    ]
                dlift[lat * line : (lat + 1) * line, :] = moved[3 * line :, lanes]
        for part in range(NLAT):
            base = part * line
            zpre = jnp.zeros((line, WIDE), F32)
            for tap in range(3):
                at = base + tap * GCOL
                zpre = zpre + mm(pooled_cat[at : at + line, :], w_eff[tap * 384 : tap * 384 + 384, :])
            sig = jax.nn.sigmoid(zpre)
            zact[base : base + line, :] = (zpre * sig).astype(BF16)
            up = mm(dlift[base : base + line, :], w_up[...], ((1,), (1,)))
            dz[base : base + line, :] = (up * (sig * (1.0 + zpre * (1.0 - sig)))).astype(BF16)
        g_up[...] = mm(zact[...], dlift[...], ((0,), (0,)))
        g_down[...] = jnp.zeros((DEPTH, WIDE), F32)
        for tap in range(3):
            at = tap * GCOL
            corr = mm(pooled_cat[at : at + CELLS, :], dz[...], ((0,), (0,)))
            high, low = split_two(corr)
            for b in range(3):
                lanes = slice(b * DEPTH, (b + 1) * DEPTH)
                table[tap * 3 + b, 0:DEPTH, :] = high[lanes]
                table[tap * 3 + b, DEPTH:, :] = low[lanes]

    pair = table[step]
    twice = jnp.concatenate([w_down[...], w_down[...]], axis=0)
    g_bot[0] = mm(twice, pair, ((0,), (0,)))
    back = mm(pair, w_bot[0], ((1,), (1,)))
    g_down[...] += back[:DEPTH] + back[DEPTH:]


def vmem():
    return pl.BlockSpec(memory_space=pltpu.VMEM)


def smem():
    return pl.BlockSpec(memory_space=pltpu.SMEM)


def shape(dims, kind):
    return jax.ShapeDtypeStruct(dims, kind)


PARAMS = dict(compiler_params=pltpu.CompilerParams(vmem_limit_bytes=56 * 1024 * 1024))


def turned(kernel):
    flipped = jnp.flip(kernel, (0, 1)).swapaxes(2, 3)
    return flipped.reshape(3, 3 * kernel.shape[3], kernel.shape[2])


def body(fine, w_enc, w_down, w_bot, w_up, w_dec, grad):
    pos = jnp.stack([lax.axis_index("lat"), lax.axis_index("lon")]).astype(jnp.int32)
    down = [(i, i + 1) for i in range(NLAT - 1)]
    up = [(t, s) for s, t in down]
    right = [(i, (i + 1) % NLON) for i in range(NLON)]
    left = [(t, s) for s, t in right]
    both = jnp.concatenate([fine, grad], axis=2)
    top = lax.ppermute(both[-2:], "lat", down)
    bot = lax.ppermute(both[:2], "lat", up)
    first = jnp.concatenate([top[:, :2], both[:, :2], bot[:, :2]], axis=0)
    last = jnp.concatenate([top[:, -2:], both[:, -2:], bot[:, -2:]], axis=0)
    low = lax.ppermute(last, "lon", right)
    high = lax.ppermute(first, "lon", left)
    strip = jnp.concatenate(
        [
            jnp.pad(high, ((1, 0), (0, 0), (0, 0))),
            jnp.zeros((21, 12, 2 * DEPTH), BF16),
            jnp.pad(low, ((0, 1), (0, 0), (0, 0))),
        ],
        axis=1,
    )
    w_eff = pl.pallas_call(
        weight_kernel,
        grid=(9,),
        in_specs=[
            pl.BlockSpec((DEPTH, WIDE), lambda i: (0, 0)),
            pl.BlockSpec((1, WIDE, WIDE), lambda i: (i, 0, 0)),
        ],
        out_specs=pl.BlockSpec((1, DEPTH, WIDE), lambda i: (i, 0, 0)),
        out_shape=shape((9, DEPTH, WIDE), BF16),
        name="weights",
    )(w_down, w_bot.reshape(9, WIDE, WIDE)).reshape(9 * DEPTH, WIDE)
    w_enc_f = w_enc.reshape(3, 3 * DEPTH, DEPTH)
    w_dec_f = w_dec.reshape(3, 3 * DEPTH, DEPTH)
    pack, hid, slope, dm, fine_cat, own_grad = pl.pallas_call(
        first_kernel,
        in_specs=[smem()] + [vmem()] * 7,
        out_specs=[vmem()] * 6,
        out_shape=[
            shape((COUNT, PACK, DEPTH), BF16),
            shape((RIM, DEPTH), BF16),
            shape((RIM, DEPTH), F32),
            shape((RIM, DEPTH), F32),
            shape((EXT, 3 * DEPTH), BF16),
            shape((OWN, DEPTH), BF16),
        ],
        scratch_shapes=[
            pltpu.VMEM((21, STRIDE, DEPTH), BF16),
            pltpu.VMEM((EXT, 3 * DEPTH), BF16),
        ],
        name="first",
        **PARAMS,
    )(pos, fine, grad, top, bot, strip, w_enc_f, turned(w_dec))
    every = lax.all_to_all(pack, AXES, 0, 0).reshape(COUNT * PACK, DEPTH)
    parts, merged_cat, dact_cat = pl.pallas_call(
        second_kernel,
        in_specs=[smem()] + [vmem()] * 8,
        out_specs=[vmem()] * 3,
        out_shape=[
            shape((COUNT * PACK, DEPTH), BF16),
            shape((RIM, 3 * DEPTH), BF16),
            shape((RIM, 3 * DEPTH), BF16),
        ],
        name="second",
        **PARAMS,
    )(pos, every, w_eff, w_up, hid, slope, dm, fine_cat, own_grad)
    spread = lax.all_to_all(parts.reshape(COUNT, PACK, DEPTH), AXES, 0, 0)
    total = spread.astype(F32).sum(axis=0).astype(BF16)
    whole = lax.all_to_all(jnp.broadcast_to(total[None], (COUNT, PACK, DEPTH)), AXES, 0, 0)
    whole = whole.reshape(COUNT * PACK, DEPTH)
    g_dec = whole[:1152].astype(F32).reshape(3, 3, DEPTH, DEPTH)
    g_enc = whole[1152:2304].astype(F32).reshape(3, 3, DEPTH, DEPTH)
    block_out, field_grad = pl.pallas_call(
        third_kernel,
        in_specs=[vmem()] * 4,
        out_specs=[vmem()] * 2,
        out_shape=[shape((ROWS, COLS, DEPTH), BF16)] * 2,
        name="third",
        **PARAMS,
    )(merged_cat, dact_cat, w_dec_f, turned(w_enc))
    g_bot, g_down, g_up = pl.pallas_call(
        coarse_kernel,
        grid=(9,),
        in_specs=[
            pl.BlockSpec((COUNT * PACK, DEPTH), lambda i: (0, 0)),
            pl.BlockSpec((9 * DEPTH, WIDE), lambda i: (0, 0)),
            pl.BlockSpec((WIDE, DEPTH), lambda i: (0, 0)),
            pl.BlockSpec((DEPTH, WIDE), lambda i: (0, 0)),
            pl.BlockSpec((1, WIDE, WIDE), lambda i: (i, 0, 0)),
        ],
        out_specs=[
            pl.BlockSpec((1, WIDE, WIDE), lambda i: (i, 0, 0)),
            pl.BlockSpec((DEPTH, WIDE), lambda i: (0, 0)),
            pl.BlockSpec((WIDE, DEPTH), lambda i: (0, 0)),
        ],
        out_shape=[
            shape((9, WIDE, WIDE), F32),
            shape((DEPTH, WIDE), F32),
            shape((WIDE, DEPTH), F32),
        ],
        scratch_shapes=[
            pltpu.VMEM(((GROW + 2) * GCOL, 3 * DEPTH), BF16),
            pltpu.VMEM((CELLS, DEPTH), BF16),
            pltpu.VMEM((CELLS, WIDE), BF16),
            pltpu.VMEM((CELLS, WIDE), BF16),
            pltpu.VMEM((9, 2 * DEPTH, WIDE), BF16),
        ],
        name="coarse",
        **PARAMS,
    )(every, w_eff, w_up, w_down, w_bot.reshape(9, WIDE, WIDE))
    return (block_out, field_grad, g_enc, g_down, g_bot.reshape(3, 3, WIDE, WIDE), g_up, g_dec)


def solution(mesh):
    return jax.shard_map(
        body,
        mesh=mesh,
        in_specs=(P("lat", "lon", None), P(), P(), P(), P(), P(), P("lat", "lon", None)),
        out_specs=(P("lat", "lon", None), P("lat", "lon", None), P(), P(), P(), P(), P()),
        check_vma=False,
    )
```

```python
import jax
import jax.numpy as jnp
from jax import lax
from jax.experimental import pallas as pl
from jax.experimental.pallas import tpu as pltpu
from jax.sharding import PartitionSpec as P

POOL = 8
AXES = ("lat", "lon")
ROWS, COLS, DEPTH = 16, 48, 128
WIDE = 512
STRIDE = 64
EXT = 21 * STRIDE
RIM = 19 * STRIDE
OWN = ROWS * STRIDE
CROW, CCOL = ROWS // POOL, COLS // POOL
NLAT, NLON = 8, 16
COUNT = NLAT * NLON
GROW, GCOL = NLAT * CROW, NLON * CCOL
CELLS = GROW * GCOL
PACK = 2 * CROW * CCOL
WIN = 16
F32 = jnp.float32
BF16 = jnp.bfloat16


def mm(left, right, contract=((1,), (0,))):
    return lax.dot_general(left, right, (contract, ((), ())), preferred_element_type=F32)


def side_by_side(flat):
    wide = flat.astype(F32)
    low = pltpu.roll(wide, 1, 0).astype(BF16)
    high = pltpu.roll(wide, flat.shape[0] - 1, 0).astype(BF16)
    return jnp.concatenate([low, flat.astype(BF16), high], axis=1)


def split_two(value):
    high = value.astype(BF16)
    return high, (value - high.astype(F32)).astype(BF16)


def rim_position(shape, dim):
    spot = lax.broadcasted_iota(jnp.int32, shape, dim)
    slot = spot & (STRIDE - 1)
    line = spot >> 6
    left = slot == STRIDE - 1
    row = jnp.where(left, line - 1, line - 2)
    col = jnp.where(left, -1, slot)
    return row, col


def row_live(row, lat):
    return jnp.logical_and(
        jnp.logical_or(row >= 0, lat > 0), jnp.logical_or(row < ROWS, lat < NLAT - 1)
    )


def mirrored(kernel, tap):
    base = 3 * (2 - tap)
    return jnp.concatenate([kernel[base + 2], kernel[base + 1], kernel[base]], axis=1)


def first_kernel(
    pos, got_inner, got_outer, strip, fine, grad, w_enc_far, w_dec_far,
    pack_out, hid_out, slope_out, dm_out, field_out,
    pack, field, grad_field, fine_cat, grad_cat, hid_here, slope_here, dm_here, w_enc, w_dec, sems,
):
    lat = pos[0]
    even = lat % 2 == 0
    fetches = [
        pltpu.make_async_copy(a, b, sems.at[5 + k])
        for k, (a, b) in enumerate(
            (
                (fine, field.at[3:19, 0:COLS, :]),
                (grad, grad_field.at[3:19, 0:COLS, :]),
                (w_enc_far, w_enc),
                (w_dec_far, w_dec),
            )
        )
    ]
    for fetch in fetches:
        fetch.start()
    sources = (field, hid_here, slope_here, dm_here, pack)
    targets = (field_out, hid_out, slope_out, dm_out, pack_out)
    copies = [
        pltpu.make_async_copy(a, b, sems.at[k]) for k, (a, b) in enumerate(zip(sources, targets))
    ]
    for part, (space, cat) in enumerate(((field, fine_cat), (grad_field, grad_cat))):
        lanes = slice(part * DEPTH, (part + 1) * DEPTH)
        space[0:1, 0:COLS, :] = jnp.zeros((1, COLS, DEPTH), BF16)
        inner = got_inner[2 * part : 2 * part + 2]
        outer = got_outer[2 * part : 2 * part + 2]
        space[1:3, 0:COLS, :] = jnp.where(even, outer, inner)
        space[19:21, 0:COLS, :] = jnp.where(even, inner, outer)
        space[:, COLS:STRIDE, :] = strip[:, :, lanes]
        fetches[part].wait()
        if part == 0:
            copies[0].start()
        cat[...] = side_by_side(space[...].reshape(EXT, DEPTH))
    act = jnp.zeros((RIM, DEPTH), F32)
    fetches[2].wait()
    for tap in range(3):
        act = act + mm(fine_cat[tap * STRIDE : tap * STRIDE + RIM, :], w_enc[tap])
    row, _ = rim_position((RIM, 1), 0)
    live = row_live(row, lat)
    sig = jax.nn.sigmoid(act)
    hid = jnp.where(live, act * sig, 0.0).astype(BF16)
    hid_here[...] = hid
    copies[1].start()
    slope_here[...] = jnp.where(live, sig * (1.0 + act * (1.0 - sig)), 0.0)
    copies[2].start()
    dm = jnp.zeros((RIM, DEPTH), F32)
    fetches[3].wait()
    for tap in range(3):
        dm = dm + mm(
            grad_cat[tap * STRIDE : tap * STRIDE + RIM, :], mirrored(w_dec, tap), ((1,), (1,))
        )
    dm_here[...] = dm
    copies[3].start()
    half = PACK // 2
    prow, pcol = rim_position((PACK, RIM), 1)
    which = lax.broadcasted_iota(jnp.int32, (PACK, RIM), 0)
    inside = (prow >= 0) & (prow < ROWS) & (pcol >= 0) & (pcol < COLS)
    cell = jnp.where(inside, (prow >> 3) * CCOL + (pcol >> 3), -1)
    take_hid = (cell == which).astype(F32).astype(BF16)
    take_dm = (inside & (cell + half == which)).astype(F32).astype(BF16)
    dm_high, dm_low = split_two(dm)
    packed = mm(take_hid, hid) * (1.0 / (POOL * POOL)) + (mm(take_dm, dm_high) + mm(take_dm, dm_low))
    packed = packed.astype(BF16)
    for peer in range(COUNT):
        pack[peer] = packed
    copies[4].start()
    for copy in copies:
        copy.wait()


def weight_kernel(w_down, w_bot, out):
    out[0] = mm(w_down[...], w_bot[0]).astype(BF16)


def third(value):
    return (value * 43) >> 8


def source_of(row, col, shift):
    inside = (row >= 0) & (row < GROW)
    col = jnp.where(col < 0, col + GCOL, col)
    col = jnp.where(col >= GCOL, col - GCOL, col)
    group = third(col)
    device = (row >> 1) * NLON + group
    return jnp.where(inside, device * PACK + shift + (row & 1) * CCOL + (col - group * CCOL), -1)


def second_kernel(
    pos, every, w_up, w_eff_far, hid_far, slope_far, dm_far, field_far, grad_far,
    parts_out, merged_out, dact_out,
    parts, w_eff, hid, slope, dm, field, own_grad, fine_cat, merged_cat, merged_here, dact_here, sems,
):
    lat, lon = pos[0], pos[1]
    fetches = [
        pltpu.make_async_copy(a, b, sems.at[k])
        for k, (a, b) in enumerate(
            (
                (w_eff_far, w_eff),
                (field_far, field),
                (hid_far, hid),
                (dm_far, dm),
                (slope_far, slope),
                (grad_far, own_grad.at[:, 0:COLS, :]),
            )
        )
    ]
    stores = [
        pltpu.make_async_copy(merged_here, merged_out, sems.at[6]),
        pltpu.make_async_copy(dact_here, dact_out, sems.at[7]),
        pltpu.make_async_copy(parts.at[0:1152, :], parts_out.at[0:1152, :], sems.at[8]),
        pltpu.make_async_copy(parts.at[1152:, :], parts_out.at[1152:, :], sems.at[9]),
    ]
    for fetch in fetches:
        fetch.start()
    own_grad[:, COLS:, :] = jnp.zeros((ROWS, STRIDE - COLS, DEPTH), BF16)
    spot = lax.broadcasted_iota(jnp.int32, (8 * WIN, 1), 0)
    line, slot = spot >> 4, spot & (WIN - 1)
    src = source_of(CROW * lat + line - 3, CCOL * lon + slot - 3, 0)
    src = jnp.where(slot < CCOL + 6, src, -1)
    spot = lax.broadcasted_iota(jnp.int32, (6 * WIN, 1), 0)
    line, slot = spot >> 4, spot & (WIN - 1)
    dsrc = source_of(CROW * lat + line - 2, CCOL * lon + slot - 2, CROW * CCOL)
    dsrc = jnp.where(slot < CCOL + 4, dsrc, -1)
    reach = 5 * NLON * PACK
    begin = jnp.clip(lat - 2, 0, NLAT - 5) * (NLON * PACK)
    near = every[pl.ds(pl.multiple_of(begin, NLON * PACK), reach), :]
    spots = lax.broadcasted_iota(jnp.int32, (8 * WIN, reach), 1) + begin
    pooled = mm((spots == src).astype(F32).astype(BF16), near)
    spots = lax.broadcasted_iota(jnp.int32, (6 * WIN, reach), 1) + begin
    dlift = mm((spots == dsrc).astype(F32).astype(BF16), near).astype(BF16)
    shifted = [pooled.astype(BF16)] + [
        pltpu.roll(pooled, 8 * WIN - step, 0).astype(BF16) for step in (1, 2)
    ]
    pooled_cat = jnp.concatenate(shifted, axis=1)
    zpre = jnp.zeros((6 * WIN, WIDE), F32)
    fetches[0].wait()
    for tap in range(3):
        zpre = zpre + mm(
            pooled_cat[tap * WIN : tap * WIN + 6 * WIN], w_eff[tap * 384 : tap * 384 + 384, :]
        )
    sig = jax.nn.sigmoid(zpre)
    zact = (zpre * sig).astype(BF16)
    dz = mm(dlift, w_up[...], ((1,), (1,))) * (sig * (1.0 + zpre * (1.0 - sig)))
    dz = dz.astype(BF16)
    lifted = mm(zact, w_up[...])
    taps = mm(dz, w_eff[...], ((1,), (1,)))
    dpool = jnp.zeros((6 * WIN, DEPTH), F32)
    for tap_a in range(3):
        for tap_b in range(3):
            spot = ((2 - tap_a) * 3 + (2 - tap_b)) * DEPTH
            turn = ((1 - tap_a) * WIN + (1 - tap_b)) % (6 * WIN)
            part = taps[:, spot : spot + DEPTH]
            dpool = dpool + (part if turn == 0 else pltpu.roll(part, turn, 0))
    dpool = dpool * (1.0 / (POOL * POOL))
    lift_high, lift_low = split_two(lifted)
    pool_high, pool_low = split_two(dpool)
    tail = jnp.zeros((2 * WIN, 2 * DEPTH), BF16)
    table = jnp.concatenate(
        [
            jnp.concatenate([lift_high, pool_high], axis=1),
            tail,
            jnp.concatenate([lift_low, pool_low], axis=1),
            tail,
        ],
        axis=0,
    )
    row, col = rim_position((RIM, 1), 0)
    home = (((row + POOL) >> 3) + 1) * WIN + ((col + POOL) >> 3) + 1
    home = jnp.where(col <= COLS, home, -1)
    cells = lax.broadcasted_iota(jnp.int32, (RIM, 256), 1) & 127
    spread = mm((cells == home).astype(F32).astype(BF16), table)
    live = row_live(row, lat)
    for fetch in fetches[1:]:
        fetch.wait()
    merged = jnp.where(live, hid[...].astype(F32) + spread[:, :DEPTH], 0.0)
    dact = (dm[...] + spread[:, DEPTH:]) * slope[...]
    merged_here[...] = merged.astype(BF16)
    stores[0].start()
    dact_here[...] = dact.astype(BF16)
    stores[1].start()
    merged_cat[...] = side_by_side(merged.astype(BF16))
    fine_cat[...] = side_by_side(field[...].reshape(EXT, DEPTH))
    slot = lax.broadcasted_iota(jnp.int32, (OWN, 1), 0) & (STRIDE - 1)
    center = dact_here[2 * STRIDE : 2 * STRIDE + OWN, :]
    own_dact = jnp.where(slot < COLS, center, jnp.zeros_like(center))
    center_grad = own_grad[...].reshape(OWN, DEPTH)
    for tap in range(3):
        start = (tap + 1) * STRIDE
        parts[tap * 384 : tap * 384 + 384, :] = mm(
            merged_cat[start : start + OWN, :], center_grad, ((0,), (0,))
        ).astype(BF16)
    stores[2].start()
    for tap in range(3):
        start = (tap + 2) * STRIDE
        parts[1152 + tap * 384 : 1152 + tap * 384 + 384, :] = mm(
            fine_cat[start : start + OWN, :], own_dact, ((0,), (0,))
        ).astype(BF16)
    stores[3].start()
    for store in stores:
        store.wait()


def third_kernel(merged, dact, w_dec, w_enc, block_out, field_grad, merged_cat, dact_cat):
    merged_cat[...] = side_by_side(merged[...])
    dact_cat[...] = side_by_side(dact[...])
    out = jnp.zeros((OWN, DEPTH), F32)
    back = jnp.zeros((OWN, DEPTH), F32)
    for tap in range(3):
        start = (tap + 1) * STRIDE
        out = out + mm(merged_cat[start : start + OWN, :], w_dec[tap])
        back = back + mm(dact_cat[start : start + OWN, :], mirrored(w_enc, tap), ((1,), (1,)))
    block_out[...] = out.astype(BF16).reshape(ROWS, STRIDE, DEPTH)[:, :COLS, :]
    field_grad[...] = back.astype(BF16).reshape(ROWS, STRIDE, DEPTH)[:, :COLS, :]


def coarse_kernel(every, w_eff, w_up, table, g_up, pooled_cat, dlift, zact, dz):
    line = 2 * GCOL
    block = NLON * PACK
    spot = lax.broadcasted_iota(jnp.int32, (4 * line, 1), 0)
    kind = (spot >= line).astype(jnp.int32) + (spot >= 2 * line).astype(jnp.int32)
    kind = kind + (spot >= 3 * line).astype(jnp.int32)
    within = spot - kind * line
    row = (within >= GCOL).astype(jnp.int32)
    col = within - row * GCOL
    col = jnp.where(kind < 3, col + kind - 1, col)
    shift = jnp.where(kind < 3, 0, CROW * CCOL)
    src = source_of(row, col, shift)
    spots = lax.broadcasted_iota(jnp.int32, (4 * line, block), 1)
    order = (spots == src).astype(F32).astype(BF16)
    edge = jnp.zeros((GCOL, 3 * DEPTH), BF16)
    pooled_cat[0:GCOL, :] = edge
    pooled_cat[(GROW + 1) * GCOL :, :] = edge
    for pair in range(NLAT // 2):
        both = jnp.concatenate(
            [every[(2 * pair + k) * block : (2 * pair + k + 1) * block, :] for k in (0, 1)],
            axis=1,
        )
        moved = mm(order, both).astype(BF16)
        for k in (0, 1):
            lat = 2 * pair + k
            lanes = slice(k * DEPTH, (k + 1) * DEPTH)
            at = GCOL + lat * line
            for b in range(3):
                pooled_cat[at : at + line, b * DEPTH : (b + 1) * DEPTH] = moved[
                    b * line : (b + 1) * line, lanes
                ]
            dlift[lat * line : (lat + 1) * line, :] = moved[3 * line :, lanes]
    for part in range(NLAT):
        base = part * line
        zpre = jnp.zeros((line, WIDE), F32)
        for tap in range(3):
            at = base + tap * GCOL
            zpre = zpre + mm(pooled_cat[at : at + line, :], w_eff[tap * 384 : tap * 384 + 384, :])
        sig = jax.nn.sigmoid(zpre)
        zact[base : base + line, :] = (zpre * sig).astype(BF16)
        up = mm(dlift[base : base + line, :], w_up[...], ((1,), (1,)))
        dz[base : base + line, :] = (up * (sig * (1.0 + zpre * (1.0 - sig)))).astype(BF16)
    g_up[...] = mm(zact[...], dlift[...], ((0,), (0,)))
    for tap in range(3):
        at = tap * GCOL
        corr = mm(pooled_cat[at : at + CELLS, :], dz[...], ((0,), (0,)))
        high, low = split_two(corr)
        for b in range(3):
            lanes = slice(b * DEPTH, (b + 1) * DEPTH)
            table[tap * 3 + b, 0:DEPTH, :] = high[lanes]
            table[tap * 3 + b, DEPTH:, :] = low[lanes]


def remainder(value):
    return value - 18 * ((value * 3641) >> 16)


def fold_kernel(spread, out):
    full = COUNT * 18
    slot = remainder(lax.broadcasted_iota(jnp.int32, (32, full), 1))
    pick = slot == lax.broadcasted_iota(jnp.int32, (32, full), 0)
    total = mm(pick.astype(F32).astype(BF16), spread[...]).astype(BF16)
    slot = remainder(lax.broadcasted_iota(jnp.int32, (full, 1), 0))
    copy = lax.broadcasted_iota(jnp.int32, (full, 32), 1) == slot
    out[...] = mm(copy.astype(F32).astype(BF16), total).astype(BF16)


def finish_kernel(whole, g_dec, g_enc):
    g_dec[...] = whole[:1152].astype(F32)
    g_enc[...] = whole[1152:].astype(F32)


def tail_kernel(table, w_down, w_bot, g_bot, g_down):
    step = pl.program_id(0)

    @pl.when(step == 0)
    def _():
        g_down[...] = jnp.zeros((DEPTH, WIDE), F32)

    pair = table[0]
    twice = jnp.concatenate([w_down[...], w_down[...]], axis=0)
    g_bot[0] = mm(twice, pair, ((0,), (0,)))
    back = mm(pair, w_bot[0], ((1,), (1,)))
    g_down[...] += back[:DEPTH] + back[DEPTH:]


def vmem():
    return pl.BlockSpec(memory_space=pltpu.VMEM)


def far():
    return pl.BlockSpec(memory_space=pltpu.HBM)


def smem():
    return pl.BlockSpec(memory_space=pltpu.SMEM)


def shape(dims, kind):
    return jax.ShapeDtypeStruct(dims, kind)


def held(value):
    return pltpu.with_memory_space_constraint(value, pltpu.HBM)


def grant(mib):
    return pltpu.CompilerParams(vmem_limit_bytes=mib * 1024 * 1024)


def body(fine, w_enc, w_down, w_bot, w_up, w_dec, grad):
    pos = jnp.stack([lax.axis_index("lat"), lax.axis_index("lon")]).astype(jnp.int32)
    inner = [(i, i ^ 1) for i in range(NLAT)]
    outer = [(i, ((i + 1) ^ 1) - 1) for i in range(1, NLAT - 1)]
    even = lax.axis_index("lat") % 2 == 0
    right = [(i, (i + 1) % NLON) for i in range(NLON)]
    left = [(t, s) for s, t in right]
    under = jnp.concatenate([fine[-2:], grad[-2:]], axis=0)
    over = jnp.concatenate([fine[:2], grad[:2]], axis=0)
    got_inner = lax.ppermute(jnp.where(even, under, over), "lat", inner)
    got_outer = lax.ppermute(jnp.where(even, over, under), "lat", outer)
    top = jnp.where(even, got_outer, got_inner)
    bot = jnp.where(even, got_inner, got_outer)

    def edge(cols):
        return jnp.concatenate(
            [
                jnp.concatenate([top[at : at + 2, cols], tile[:, cols], bot[at : at + 2, cols]], axis=0)
                for at, tile in ((0, fine), (2, grad))
            ],
            axis=2,
        )

    first = edge(slice(0, 2))
    last = edge(slice(COLS - 2, COLS))
    high = lax.ppermute(first, "lon", left)
    low = lax.ppermute(last, "lon", right)
    strip = jnp.concatenate(
        [
            jnp.pad(high, ((1, 0), (0, 0), (0, 0))),
            jnp.zeros((21, 12, 2 * DEPTH), BF16),
            jnp.pad(low, ((0, 1), (0, 0), (0, 0))),
        ],
        axis=1,
    )
    w_eff = pl.pallas_call(
        weight_kernel,
        grid=(9,),
        in_specs=[
            pl.BlockSpec((DEPTH, WIDE), lambda i: (0, 0)),
            pl.BlockSpec((1, WIDE, WIDE), lambda i: (i, 0, 0)),
        ],
        out_specs=pl.BlockSpec((1, DEPTH, WIDE), lambda i: (i, 0, 0)),
        out_shape=shape((9, DEPTH, WIDE), BF16),
        name="weights",
        compiler_params=grant(56),
    )(w_down, w_bot.reshape(9, WIDE, WIDE)).reshape(9 * DEPTH, WIDE)
    w_enc_f = w_enc.reshape(3, 3 * DEPTH, DEPTH)
    w_dec_f = w_dec.reshape(3, 3 * DEPTH, DEPTH)
    pack, hid, slope, dm, field = pl.pallas_call(
        first_kernel,
        in_specs=[smem()] + [vmem()] * 3 + [far()] * 4,
        out_specs=[far()] * 5,
        out_shape=[
            pltpu.HBM((COUNT, PACK, DEPTH), BF16),
            pltpu.HBM((RIM, DEPTH), BF16),
            pltpu.HBM((RIM, DEPTH), F32),
            pltpu.HBM((RIM, DEPTH), F32),
            pltpu.HBM((21, STRIDE, DEPTH), BF16),
        ],
        scratch_shapes=[
            pltpu.VMEM((COUNT, PACK, DEPTH), BF16),
            pltpu.VMEM((21, STRIDE, DEPTH), BF16),
            pltpu.VMEM((21, STRIDE, DEPTH), BF16),
            pltpu.VMEM((EXT, 3 * DEPTH), BF16),
            pltpu.VMEM((EXT, 3 * DEPTH), BF16),
            pltpu.VMEM((RIM, DEPTH), BF16),
            pltpu.VMEM((RIM, DEPTH), F32),
            pltpu.VMEM((RIM, DEPTH), F32),
            pltpu.VMEM((3, 3 * DEPTH, DEPTH), BF16),
            pltpu.VMEM((9, DEPTH, DEPTH), BF16),
            pltpu.SemaphoreType.DMA((9,)),
        ],
        name="first",
        compiler_params=grant(30),
    )(
        pos, got_inner, got_outer, strip,
        *(held(x) for x in (fine, grad, w_enc_f, w_dec.reshape(9, DEPTH, DEPTH))),
    )
    every = lax.all_to_all(pack, AXES, 0, 0).reshape(COUNT * PACK, DEPTH)
    parts, merged, dact = pl.pallas_call(
        second_kernel,
        in_specs=[smem(), vmem(), vmem()] + [far()] * 6,
        out_specs=[far()] * 3,
        out_shape=[
            pltpu.HBM((2304, DEPTH), BF16),
            pltpu.HBM((RIM, DEPTH), BF16),
            pltpu.HBM((RIM, DEPTH), BF16),
        ],
        scratch_shapes=[
            pltpu.VMEM((2304, DEPTH), BF16),
            pltpu.VMEM((9 * DEPTH, WIDE), BF16),
            pltpu.VMEM((RIM, DEPTH), BF16),
            pltpu.VMEM((RIM, DEPTH), F32),
            pltpu.VMEM((RIM, DEPTH), F32),
            pltpu.VMEM((21, STRIDE, DEPTH), BF16),
            pltpu.VMEM((ROWS, STRIDE, DEPTH), BF16),
            pltpu.VMEM((EXT, 3 * DEPTH), BF16),
            pltpu.VMEM((RIM, 3 * DEPTH), BF16),
            pltpu.VMEM((RIM, DEPTH), BF16),
            pltpu.VMEM((RIM, DEPTH), BF16),
            pltpu.SemaphoreType.DMA((10,)),
        ],
        name="second",
        compiler_params=grant(30),
    )(pos, every, w_up, *(held(x) for x in (w_eff, hid, slope, dm, field, grad)))
    parts, later, merged, dact = lax.optimization_barrier(
        (parts, every, merged, dact)
    )
    spread = lax.all_to_all(parts.reshape(COUNT, 9, 2, DEPTH), AXES, 0, 0)
    table, g_up = pl.pallas_call(
        coarse_kernel,
        in_specs=[vmem()] * 3,
        out_specs=[vmem()] * 2,
        out_shape=[
            shape((9, 2 * DEPTH, WIDE), BF16),
            shape((WIDE, DEPTH), F32),
        ],
        scratch_shapes=[
            pltpu.VMEM(((GROW + 2) * GCOL, 3 * DEPTH), BF16),
            pltpu.VMEM((CELLS, DEPTH), BF16),
            pltpu.VMEM((CELLS, WIDE), BF16),
            pltpu.VMEM((CELLS, WIDE), BF16),
        ],
        name="coarse",
        compiler_params=grant(56),
    )(later, w_eff, w_up)
    block_out, field_grad = pl.pallas_call(
        third_kernel,
        in_specs=[vmem()] * 4,
        out_specs=[vmem()] * 2,
        out_shape=[shape((ROWS, COLS, DEPTH), BF16)] * 2,
        scratch_shapes=[pltpu.VMEM((RIM, 3 * DEPTH), BF16)] * 2,
        name="third",
        compiler_params=grant(56),
    )(merged, dact, w_dec_f, w_enc.reshape(9, DEPTH, DEPTH))
    spread, table, block_out = lax.optimization_barrier((spread, table, block_out))
    total = pl.pallas_call(
        fold_kernel,
        in_specs=[vmem()],
        out_specs=vmem(),
        out_shape=pltpu.VMEM((2304, DEPTH), BF16),
        name="fold",
        compiler_params=grant(8),
    )(spread.reshape(2304, DEPTH))
    total, table = lax.optimization_barrier((total, table))
    whole = lax.all_to_all(total.reshape(COUNT, 9, 2, DEPTH), AXES, 0, 0)
    g_bot, g_down = pl.pallas_call(
        tail_kernel,
        grid=(9,),
        in_specs=[
            pl.BlockSpec((1, 2 * DEPTH, WIDE), lambda i: (i, 0, 0)),
            pl.BlockSpec((DEPTH, WIDE), lambda i: (0, 0)),
            pl.BlockSpec((1, WIDE, WIDE), lambda i: (i, 0, 0)),
        ],
        out_specs=[
            pl.BlockSpec((1, WIDE, WIDE), lambda i: (i, 0, 0)),
            pl.BlockSpec((DEPTH, WIDE), lambda i: (0, 0)),
        ],
        out_shape=[shape((9, WIDE, WIDE), F32), shape((DEPTH, WIDE), F32)],
        name="tail",
        compiler_params=grant(56),
    )(table, w_down, w_bot.reshape(9, WIDE, WIDE))
    whole, g_bot = lax.optimization_barrier((whole, g_bot))
    g_dec, g_enc = pl.pallas_call(
        finish_kernel,
        in_specs=[vmem()],
        out_specs=[vmem()] * 2,
        out_shape=[shape((1152, DEPTH), F32)] * 2,
        name="finish",
        compiler_params=grant(6),
    )(whole.reshape(2304, DEPTH))
    g_dec = g_dec.reshape(3, 3, DEPTH, DEPTH)
    g_enc = g_enc.reshape(3, 3, DEPTH, DEPTH)
    return (block_out, field_grad, g_enc, g_down, g_bot.reshape(3, 3, WIDE, WIDE), g_up, g_dec)


def solution(mesh):
    return jax.shard_map(
        body,
        mesh=mesh,
        in_specs=(P("lat", "lon", None), P(), P(), P(), P(), P(), P("lat", "lon", None)),
        out_specs=(P("lat", "lon", None), P("lat", "lon", None), P(), P(), P(), P(), P()),
        check_vma=False,
    )
```

```python
import jax
import jax.numpy as jnp
from jax import lax
from jax.experimental import pallas as pl
from jax.experimental.pallas import tpu as pltpu
from jax.sharding import Mesh
from jax.sharding import PartitionSpec as P

POOL = 8
LON = ("pair", "core")
PEERS = ("lat", "pair")
EVERYONE = ("lat", "pair", "core")
ROWS, COLS, DEPTH = 16, 48, 128
WIDE = 512
STRIDE = 64
EXT = 21 * STRIDE
RIM = 19 * STRIDE
OWN = ROWS * STRIDE
CROW, CCOL = ROWS // POOL, COLS // POOL
NLAT, NLON = 8, 16
COUNT = NLAT * NLON // 2
HALF = COUNT * 18
GROW, GCOL = NLAT * CROW, NLON * CCOL
CELLS = GROW * GCOL
PACK = 2 * CROW * CCOL
WIN = 16
F32 = jnp.float32
BF16 = jnp.bfloat16


def mm(left, right, contract=((1,), (0,))):
    return lax.dot_general(left, right, (contract, ((), ())), preferred_element_type=F32)


def side_by_side(flat):
    wide = flat.astype(F32)
    low = pltpu.roll(wide, 1, 0).astype(BF16)
    high = pltpu.roll(wide, flat.shape[0] - 1, 0).astype(BF16)
    return jnp.concatenate([low, flat.astype(BF16), high], axis=1)


def split_two(value):
    high = value.astype(BF16)
    return high, (value - high.astype(F32)).astype(BF16)


def rim_position(shape, dim):
    spot = lax.broadcasted_iota(jnp.int32, shape, dim)
    slot = spot & (STRIDE - 1)
    line = spot >> 6
    left = slot == STRIDE - 1
    row = jnp.where(left, line - 1, line - 2)
    col = jnp.where(left, -1, slot)
    return row, col


def row_live(row, lat):
    return jnp.logical_and(
        jnp.logical_or(row >= 0, lat > 0), jnp.logical_or(row < ROWS, lat < NLAT - 1)
    )


def mirrored(kernel, tap):
    base = 3 * (2 - tap)
    return jnp.concatenate([kernel[base + 2], kernel[base + 1], kernel[base]], axis=1)


def first_kernel(
    pos, got_inner, got_outer, strip, fine, grad, w_enc_far, w_dec_far,
    pack_out, hid_out, slope_out, dm_out, field_out,
    pack, field, grad_field, fine_cat, grad_cat, hid_here, slope_here, dm_here, w_enc, w_dec, sems,
):
    lat = pos[0]
    even = lat % 2 == 0
    fetches = [
        pltpu.make_async_copy(a, b, sems.at[5 + k])
        for k, (a, b) in enumerate(
            (
                (fine, field.at[3:19, 0:COLS, :]),
                (grad, grad_field.at[3:19, 0:COLS, :]),
                (w_enc_far, w_enc),
                (w_dec_far, w_dec),
            )
        )
    ]
    for fetch in fetches:
        fetch.start()
    sources = (field, hid_here, slope_here, dm_here, pack)
    targets = (field_out, hid_out, slope_out, dm_out, pack_out)
    copies = [
        pltpu.make_async_copy(a, b, sems.at[k]) for k, (a, b) in enumerate(zip(sources, targets))
    ]
    for part, (space, cat) in enumerate(((field, fine_cat), (grad_field, grad_cat))):
        lanes = slice(part * DEPTH, (part + 1) * DEPTH)
        space[0:1, 0:COLS, :] = jnp.zeros((1, COLS, DEPTH), BF16)
        inner = got_inner[2 * part : 2 * part + 2]
        outer = got_outer[2 * part : 2 * part + 2]
        space[1:3, 0:COLS, :] = jnp.where(even, outer, inner)
        space[19:21, 0:COLS, :] = jnp.where(even, inner, outer)
        space[:, COLS:STRIDE, :] = strip[:, :, lanes]
        fetches[part].wait()
        if part == 0:
            copies[0].start()
        cat[...] = side_by_side(space[...].reshape(EXT, DEPTH))
    act = jnp.zeros((RIM, DEPTH), F32)
    fetches[2].wait()
    for tap in range(3):
        act = act + mm(fine_cat[tap * STRIDE : tap * STRIDE + RIM, :], w_enc[tap])
    row, _ = rim_position((RIM, 1), 0)
    live = row_live(row, lat)
    sig = jax.nn.sigmoid(act)
    hid = jnp.where(live, act * sig, 0.0).astype(BF16)
    hid_here[...] = hid
    copies[1].start()
    slope_here[...] = jnp.where(live, sig * (1.0 + act * (1.0 - sig)), 0.0)
    copies[2].start()
    dm = jnp.zeros((RIM, DEPTH), F32)
    fetches[3].wait()
    for tap in range(3):
        dm = dm + mm(
            grad_cat[tap * STRIDE : tap * STRIDE + RIM, :], mirrored(w_dec, tap), ((1,), (1,))
        )
    dm_here[...] = dm
    copies[3].start()
    half = PACK // 2
    prow, pcol = rim_position((PACK, RIM), 1)
    which = lax.broadcasted_iota(jnp.int32, (PACK, RIM), 0)
    inside = (prow >= 0) & (prow < ROWS) & (pcol >= 0) & (pcol < COLS)
    cell = jnp.where(inside, (prow >> 3) * CCOL + (pcol >> 3), -1)
    take_hid = (cell == which).astype(F32).astype(BF16)
    take_dm = (inside & (cell + half == which)).astype(F32).astype(BF16)
    dm_high, dm_low = split_two(dm)
    packed = mm(take_hid, hid) * (1.0 / (POOL * POOL)) + (mm(take_dm, dm_high) + mm(take_dm, dm_low))
    packed = packed.astype(BF16)
    for peer in range(COUNT):
        pack[peer] = packed
    copies[4].start()
    for copy in copies:
        copy.wait()


def weight_kernel(w_down, w_bot_far, out_far, w_bot, out, sems):
    fetches = [pltpu.make_async_copy(w_bot_far.at[k], w_bot.at[k], sems.at[k]) for k in range(9)]
    stores = [pltpu.make_async_copy(out.at[k], out_far.at[k], sems.at[9 + k]) for k in range(9)]
    for fetch in fetches:
        fetch.start()
    for k in range(9):
        fetches[k].wait()
        out[k] = mm(w_down[...], w_bot[k]).astype(BF16)
        stores[k].start()
    for store in stores:
        store.wait()


def third(value):
    return (value * 43) >> 8


def source_of(row, col, shift, core, first, lats):
    inside = (row >= 0) & (row < GROW)
    col = jnp.where(col < 0, col + GCOL, col)
    col = jnp.where(col >= GCOL, col - GCOL, col)
    group = third(col)
    place = ((row >> 1) - first) * (NLON // 2) + (group >> 1)
    half = jnp.where((group & 1) == core, 0, lats * (NLON // 2) * PACK)
    return jnp.where(
        inside, half + place * PACK + shift + (row & 1) * CCOL + (col - group * CCOL), -1
    )


def second_kernel(
    pos, every, every_far, w_up, w_eff_far, hid_far, slope_far, dm_far, field_far, grad_far,
    keep_out, give_out, merged_out, dact_out,
    keep, give, w_eff, hid, slope, dm, field, own_grad, fine_cat, merged_cat, merged_here, dact_here, sems,
):
    lat, lon, core = pos[0], pos[1], pos[2]
    fetches = [
        pltpu.make_async_copy(a, b, sems.at[k])
        for k, (a, b) in enumerate(
            (
                (w_eff_far, w_eff),
                (field_far, field),
                (hid_far, hid),
                (dm_far, dm),
                (slope_far, slope),
                (grad_far, own_grad.at[:, 0:COLS, :]),
            )
        )
    ]
    stores = [
        pltpu.make_async_copy(merged_here, merged_out, sems.at[6]),
        pltpu.make_async_copy(dact_here, dact_out, sems.at[7]),
        pltpu.make_async_copy(give, give_out, sems.at[8]),
        pltpu.make_async_copy(keep, keep_out, sems.at[9]),
    ]
    for fetch in fetches:
        fetch.start()
    own_grad[:, COLS:, :] = jnp.zeros((ROWS, STRIDE - COLS, DEPTH), BF16)
    lats = 5
    first = jnp.clip(lat - 2, 0, NLAT - lats)
    spot = lax.broadcasted_iota(jnp.int32, (8 * WIN, 1), 0)
    line, slot = spot >> 4, spot & (WIN - 1)
    src = source_of(CROW * lat + line - 3, CCOL * lon + slot - 3, 0, core, first, lats)
    src = jnp.where(slot < CCOL + 6, src, -1)
    spot = lax.broadcasted_iota(jnp.int32, (6 * WIN, 1), 0)
    line, slot = spot >> 4, spot & (WIN - 1)
    dsrc = source_of(
        CROW * lat + line - 2, CCOL * lon + slot - 2, CROW * CCOL, core, first, lats
    )
    dsrc = jnp.where(slot < CCOL + 4, dsrc, -1)
    strip = NLON // 2 * PACK
    begin = pl.multiple_of(first * strip, strip)
    reach = lats * strip
    near = jnp.concatenate(
        [every[pl.ds(begin, reach), :], every_far[pl.ds(begin, reach), :]], axis=0
    )
    spots = lax.broadcasted_iota(jnp.int32, (8 * WIN, 2 * reach), 1)
    pooled = mm((spots == src).astype(F32).astype(BF16), near)
    spots = lax.broadcasted_iota(jnp.int32, (6 * WIN, 2 * reach), 1)
    dlift = mm((spots == dsrc).astype(F32).astype(BF16), near).astype(BF16)
    shifted = [pooled.astype(BF16)] + [
        pltpu.roll(pooled, 8 * WIN - step, 0).astype(BF16) for step in (1, 2)
    ]
    pooled_cat = jnp.concatenate(shifted, axis=1)
    zpre = jnp.zeros((6 * WIN, WIDE), F32)
    fetches[0].wait()
    for tap in range(3):
        zpre = zpre + mm(
            pooled_cat[tap * WIN : tap * WIN + 6 * WIN], w_eff[tap * 384 : tap * 384 + 384, :]
        )
    sig = jax.nn.sigmoid(zpre)
    zact = (zpre * sig).astype(BF16)
    dz = mm(dlift, w_up[...], ((1,), (1,))) * (sig * (1.0 + zpre * (1.0 - sig)))
    dz = dz.astype(BF16)
    lifted = mm(zact, w_up[...])
    taps = mm(dz, w_eff[...], ((1,), (1,)))
    dpool = jnp.zeros((6 * WIN, DEPTH), F32)
    for tap_a in range(3):
        for tap_b in range(3):
            spot = ((2 - tap_a) * 3 + (2 - tap_b)) * DEPTH
            turn = ((1 - tap_a) * WIN + (1 - tap_b)) % (6 * WIN)
            part = taps[:, spot : spot + DEPTH]
            dpool = dpool + (part if turn == 0 else pltpu.roll(part, turn, 0))
    dpool = dpool * (1.0 / (POOL * POOL))
    lift_high, lift_low = split_two(lifted)
    pool_high, pool_low = split_two(dpool)
    tail = jnp.zeros((2 * WIN, 2 * DEPTH), BF16)
    table = jnp.concatenate(
        [
            jnp.concatenate([lift_high, pool_high], axis=1),
            tail,
            jnp.concatenate([lift_low, pool_low], axis=1),
            tail,
        ],
        axis=0,
    )
    row, col = rim_position((RIM, 1), 0)
    home = (((row + POOL) >> 3) + 1) * WIN + ((col + POOL) >> 3) + 1
    home = jnp.where(col <= COLS, home, -1)
    cells = lax.broadcasted_iota(jnp.int32, (RIM, 256), 1) & 127
    spread = mm((cells == home).astype(F32).astype(BF16), table)
    live = row_live(row, lat)
    for fetch in fetches[1:]:
        fetch.wait()
    merged = jnp.where(live, hid[...].astype(F32) + spread[:, :DEPTH], 0.0)
    dact = (dm[...] + spread[:, DEPTH:]) * slope[...]
    merged_here[...] = merged.astype(BF16)
    stores[0].start()
    dact_here[...] = dact.astype(BF16)
    stores[1].start()
    merged_cat[...] = side_by_side(merged.astype(BF16))
    fine_cat[...] = side_by_side(field[...].reshape(EXT, DEPTH))
    slot = lax.broadcasted_iota(jnp.int32, (OWN, 1), 0) & (STRIDE - 1)
    center = dact_here[2 * STRIDE : 2 * STRIDE + OWN, :]
    own_dact = jnp.where(slot < COLS, center, jnp.zeros_like(center))
    center_grad = own_grad[...].reshape(OWN, DEPTH)
    zero = core == 0
    for tap in range(3):
        rows = slice(tap * 384, tap * 384 + 384)
        start = (tap + 1) * STRIDE
        dec = mm(merged_cat[start : start + OWN, :], center_grad, ((0,), (0,))).astype(BF16)
        start = (tap + 2) * STRIDE
        enc = mm(fine_cat[start : start + OWN, :], own_dact, ((0,), (0,))).astype(BF16)
        give[rows, :] = jnp.where(zero, enc, dec)
        keep[rows, :] = jnp.where(zero, dec, enc)
    stores[2].start()
    stores[3].start()
    for store in stores:
        store.wait()


def coarse_kernel(
    pos, w_up, every_out, every_far_out, w_eff_out, table_out, g_up,
    every, every_far, w_eff, table, pooled_cat, dlift, zact, dz, sems,
):
    fetches = [
        pltpu.make_async_copy(a, b, sems.at[k])
        for k, (a, b) in enumerate(
            ((every_out, every), (every_far_out, every_far), (w_eff_out, w_eff))
        )
    ]
    stores = [
        pltpu.make_async_copy(
            table.at[3 * k : 3 * k + 3], table_out.at[3 * k : 3 * k + 3], sems.at[3 + k]
        )
        for k in range(3)
    ]
    for fetch in fetches:
        fetch.start()
    line = 2 * GCOL
    core = pos[2]
    strip = NLON // 2 * PACK
    spot = lax.broadcasted_iota(jnp.int32, (4 * line, 1), 0)
    kind = (spot >= line).astype(jnp.int32) + (spot >= 2 * line).astype(jnp.int32)
    kind = kind + (spot >= 3 * line).astype(jnp.int32)
    within = spot - kind * line
    row = (within >= GCOL).astype(jnp.int32)
    col = within - row * GCOL
    col = jnp.where(kind < 3, col + kind - 1, col)
    shift = jnp.where(kind < 3, 0, CROW * CCOL)
    src = source_of(row, col, shift, core, 0, 1)
    spots = lax.broadcasted_iota(jnp.int32, (4 * line, 2 * strip), 1)
    order = (spots == src).astype(F32).astype(BF16)
    edge = jnp.zeros((GCOL, 3 * DEPTH), BF16)
    pooled_cat[0:GCOL, :] = edge
    pooled_cat[(GROW + 1) * GCOL :, :] = edge
    fetches[0].wait()
    fetches[1].wait()
    for pair in range(NLAT // 2):
        both = jnp.concatenate(
            [
                jnp.concatenate(
                    [part[(2 * pair + k) * strip : (2 * pair + k + 1) * strip, :] for k in (0, 1)],
                    axis=1,
                )
                for part in (every, every_far)
            ],
            axis=0,
        )
        moved = mm(order, both).astype(BF16)
        for k in (0, 1):
            lat = 2 * pair + k
            lanes = slice(k * DEPTH, (k + 1) * DEPTH)
            at = GCOL + lat * line
            for b in range(3):
                pooled_cat[at : at + line, b * DEPTH : (b + 1) * DEPTH] = moved[
                    b * line : (b + 1) * line, lanes
                ]
            dlift[lat * line : (lat + 1) * line, :] = moved[3 * line :, lanes]
    fetches[2].wait()
    rows = 384
    for part in range(CELLS // rows):
        base = part * rows
        spread = jnp.concatenate(
            [pooled_cat[base + tap * GCOL : base + tap * GCOL + rows, :] for tap in range(3)], axis=1
        )
        zpre = mm(spread, w_eff[...])
        sig = jax.nn.sigmoid(zpre)
        zact[base : base + rows, :] = (zpre * sig).astype(BF16)
        up = mm(dlift[base : base + rows, :], w_up[...], ((1,), (1,)))
        dz[GCOL + base : GCOL + base + rows, :] = (up * (sig * (1.0 + zpre * (1.0 - sig)))).astype(BF16)
    blank = jnp.zeros((GCOL, WIDE), BF16)
    dz[0:GCOL, :] = blank
    dz[GCOL + CELLS :, :] = blank
    lying = pooled_cat[GCOL : GCOL + CELLS, :].T
    for tap in range(3):
        at = (2 - tap) * GCOL
        corr = mm(lying, dz[at : at + CELLS, :]).astype(BF16)
        table[3 * tap : 3 * tap + 3] = corr.reshape(3, DEPTH, WIDE)
        stores[tap].start()
    g_up[...] = mm(dlift[...].T, zact[...]).T
    for store in stores:
        store.wait()


def remainder(value):
    return value - 18 * ((value * 3641) >> 16)


def add_kernel(got, keep_far, out, keep, sems):
    fetch = pltpu.make_async_copy(keep_far, keep, sems.at[0])
    fetch.start()
    fetch.wait()
    out[...] = (keep[...].astype(F32) + got[...].astype(F32)).astype(BF16)


def fold_kernel(spread, out):
    slot = remainder(lax.broadcasted_iota(jnp.int32, (32, HALF), 1))
    pick = slot == lax.broadcasted_iota(jnp.int32, (32, HALF), 0)
    total = mm(pick.astype(F32).astype(BF16), spread[...]).astype(BF16)
    slot = remainder(lax.broadcasted_iota(jnp.int32, (2 * HALF, 1), 0))
    copy = lax.broadcasted_iota(jnp.int32, (2 * HALF, 32), 1) == slot
    out[...] = mm(copy.astype(F32).astype(BF16), total).astype(BF16)


def finish_kernel(whole, g_dec, g_enc):
    row = lax.broadcasted_iota(jnp.int32, (144, 1), 0)
    half = (row >= 72).astype(jnp.int32)
    rest = row - 72 * half
    step = sum((rest >= 18 * k).astype(jnp.int32) for k in (1, 2, 3))
    src = rest + 18 * step + 18 * half
    order = (lax.broadcasted_iota(jnp.int32, (144, 144), 1) == src).astype(F32).astype(BF16)
    for block in range(16):
        rows = mm(order, whole[144 * block : 144 * block + 144, :])
        g_dec[72 * block : 72 * block + 72, :] = rows[:72]
        g_enc[72 * block : 72 * block + 72, :] = rows[72:]


def tail_kernel(
    w_down, table_far, merged_far, dact_far, w_dec_far, w_enc_far, w_bot_far,
    g_bot_far, block_far, back_far, g_down,
    table, merged, dact, w_dec, w_enc, w_bot, g_bot, merged_cat, dact_cat, block, back, sems,
):
    fetches = [
        pltpu.make_async_copy(a, b, sems.at[18 + k])
        for k, (a, b) in enumerate(
            (
                (table_far, table),
                (merged_far, merged),
                (dact_far, dact),
                (w_dec_far, w_dec),
                (w_enc_far, w_enc),
            )
        )
    ]
    loads = [pltpu.make_async_copy(w_bot_far.at[k], w_bot.at[k], sems.at[k]) for k in range(9)]
    stores = [pltpu.make_async_copy(g_bot.at[k], g_bot_far.at[k], sems.at[9 + k]) for k in range(9)]
    stores.append(pltpu.make_async_copy(block.at[:, 0:COLS, :], block_far, sems.at[23]))
    stores.append(pltpu.make_async_copy(back.at[:, 0:COLS, :], back_far, sems.at[24]))
    for fetch in fetches:
        fetch.start()
    for load in loads:
        load.start()
    fetches[0].wait()
    for k in range(9):
        g_bot[k] = mm(w_down[...], table[k], ((0,), (0,)))
        stores[k].start()
    for fetch in fetches[1:]:
        fetch.wait()
    merged_cat[...] = side_by_side(merged[...])
    dact_cat[...] = side_by_side(dact[...])
    fore = jnp.zeros((OWN, DEPTH), F32)
    aft = jnp.zeros((OWN, DEPTH), F32)
    for tap in range(3):
        start = (tap + 1) * STRIDE
        fore = fore + mm(merged_cat[start : start + OWN, :], w_dec[tap])
        aft = aft + mm(dact_cat[start : start + OWN, :], mirrored(w_enc, tap), ((1,), (1,)))
    block[...] = fore.astype(BF16).reshape(ROWS, STRIDE, DEPTH)
    stores[9].start()
    back[...] = aft.astype(BF16).reshape(ROWS, STRIDE, DEPTH)
    stores[10].start()
    total = jnp.zeros((DEPTH, WIDE), F32)
    for k in range(9):
        loads[k].wait()
        total = total + mm(table[k], w_bot[k], ((1,), (1,)))
    g_down[...] = total
    for store in stores:
        store.wait()


def vmem():
    return pl.BlockSpec(memory_space=pltpu.VMEM)


def far():
    return pl.BlockSpec(memory_space=pltpu.HBM)


def smem():
    return pl.BlockSpec(memory_space=pltpu.SMEM)


def shape(dims, kind):
    return jax.ShapeDtypeStruct(dims, kind)


def held(value):
    return pltpu.with_memory_space_constraint(value, pltpu.HBM)


def grant(mib):
    return pltpu.CompilerParams(vmem_limit_bytes=mib * 1024 * 1024)


def body(fine, w_enc, w_down, w_bot, w_up, w_dec, grad):
    pos = jnp.stack([lax.axis_index("lat"), lax.axis_index(LON), lax.axis_index("core")])
    pos = pos.astype(jnp.int32)
    swap = [(0, 1), (1, 0)]
    inner = [(i, i ^ 1) for i in range(NLAT)]
    outer = [(i, ((i + 1) ^ 1) - 1) for i in range(1, NLAT - 1)]
    even = lax.axis_index("lat") % 2 == 0
    right = [(i, (i + 1) % NLON) for i in range(NLON)]
    left = [(t, s) for s, t in right]
    under = jnp.concatenate([fine[-2:], grad[-2:]], axis=0)
    over = jnp.concatenate([fine[:2], grad[:2]], axis=0)
    got_inner = lax.ppermute(jnp.where(even, under, over), "lat", inner)
    got_outer = lax.ppermute(jnp.where(even, over, under), "lat", outer)
    top = jnp.where(even, got_outer, got_inner)
    bot = jnp.where(even, got_inner, got_outer)

    def edge(cols):
        return jnp.concatenate(
            [
                jnp.concatenate([top[at : at + 2, cols], tile[:, cols], bot[at : at + 2, cols]], axis=0)
                for at, tile in ((0, fine), (2, grad))
            ],
            axis=2,
        )

    first = edge(slice(0, 2))
    last = edge(slice(COLS - 2, COLS))
    high = lax.ppermute(first, LON, left)
    low = lax.ppermute(last, LON, right)
    strip = jnp.concatenate(
        [
            jnp.pad(high, ((1, 0), (0, 0), (0, 0))),
            jnp.zeros((21, 12, 2 * DEPTH), BF16),
            jnp.pad(low, ((0, 1), (0, 0), (0, 0))),
        ],
        axis=1,
    )
    w_enc_f = w_enc.reshape(3, 3 * DEPTH, DEPTH)
    w_dec_f = w_dec.reshape(3, 3 * DEPTH, DEPTH)
    pack, hid, slope, dm, field = pl.pallas_call(
        first_kernel,
        in_specs=[smem()] + [vmem()] * 3 + [far()] * 4,
        out_specs=[far()] * 5,
        out_shape=[
            pltpu.HBM((COUNT, PACK, DEPTH), BF16),
            pltpu.HBM((RIM, DEPTH), BF16),
            pltpu.HBM((RIM, DEPTH), F32),
            pltpu.HBM((RIM, DEPTH), F32),
            pltpu.HBM((21, STRIDE, DEPTH), BF16),
        ],
        scratch_shapes=[
            pltpu.VMEM((COUNT, PACK, DEPTH), BF16),
            pltpu.VMEM((21, STRIDE, DEPTH), BF16),
            pltpu.VMEM((21, STRIDE, DEPTH), BF16),
            pltpu.VMEM((EXT, 3 * DEPTH), BF16),
            pltpu.VMEM((EXT, 3 * DEPTH), BF16),
            pltpu.VMEM((RIM, DEPTH), BF16),
            pltpu.VMEM((RIM, DEPTH), F32),
            pltpu.VMEM((RIM, DEPTH), F32),
            pltpu.VMEM((3, 3 * DEPTH, DEPTH), BF16),
            pltpu.VMEM((9, DEPTH, DEPTH), BF16),
            pltpu.SemaphoreType.DMA((9,)),
        ],
        name="first",
        compiler_params=grant(30),
    )(
        pos, got_inner, got_outer, strip,
        *(held(x) for x in (fine, grad, w_enc_f, w_dec.reshape(9, DEPTH, DEPTH))),
    )
    pack, early = lax.optimization_barrier((pack, w_down))
    every = lax.all_to_all(pack, PEERS, 0, 0).reshape(COUNT * PACK, DEPTH)
    w_eff = pl.pallas_call(
        weight_kernel,
        in_specs=[vmem(), far()],
        out_specs=far(),
        out_shape=pltpu.HBM((9, DEPTH, WIDE), BF16),
        scratch_shapes=[
            pltpu.VMEM((9, WIDE, WIDE), BF16),
            pltpu.VMEM((9, DEPTH, WIDE), BF16),
            pltpu.SemaphoreType.DMA((18,)),
        ],
        name="weights",
        compiler_params=grant(56),
    )(early, held(w_bot.reshape(9, WIDE, WIDE))).reshape(9 * DEPTH, WIDE)
    every, w_eff = lax.optimization_barrier((every, w_eff))
    every_far = lax.ppermute(every, "core", swap)
    keep, give, merged, dact = pl.pallas_call(
        second_kernel,
        in_specs=[smem(), vmem(), vmem(), vmem()] + [far()] * 6,
        out_specs=[far()] * 4,
        out_shape=[
            pltpu.HBM((HALF, DEPTH), BF16),
            pltpu.HBM((HALF, DEPTH), BF16),
            pltpu.HBM((RIM, DEPTH), BF16),
            pltpu.HBM((RIM, DEPTH), BF16),
        ],
        scratch_shapes=[
            pltpu.VMEM((HALF, DEPTH), BF16),
            pltpu.VMEM((HALF, DEPTH), BF16),
            pltpu.VMEM((9 * DEPTH, WIDE), BF16),
            pltpu.VMEM((RIM, DEPTH), BF16),
            pltpu.VMEM((RIM, DEPTH), F32),
            pltpu.VMEM((RIM, DEPTH), F32),
            pltpu.VMEM((21, STRIDE, DEPTH), BF16),
            pltpu.VMEM((ROWS, STRIDE, DEPTH), BF16),
            pltpu.VMEM((EXT, 3 * DEPTH), BF16),
            pltpu.VMEM((RIM, 3 * DEPTH), BF16),
            pltpu.VMEM((RIM, DEPTH), BF16),
            pltpu.VMEM((RIM, DEPTH), BF16),
            pltpu.SemaphoreType.DMA((10,)),
        ],
        name="second",
        compiler_params=grant(30),
    )(pos, every, every_far, w_up, *(held(x) for x in (w_eff, hid, slope, dm, field, grad)))
    keep, give, every, every_far, merged, dact = lax.optimization_barrier(
        (keep, give, every, every_far, merged, dact)
    )
    got = lax.ppermute(give, "core", swap)
    half = pl.pallas_call(
        add_kernel,
        in_specs=[vmem(), far()],
        out_specs=vmem(),
        out_shape=shape((HALF, DEPTH), BF16),
        scratch_shapes=[pltpu.VMEM((HALF, DEPTH), BF16), pltpu.SemaphoreType.DMA((1,))],
        name="add",
        compiler_params=grant(6),
    )(got, held(keep))
    half, every, every_far = lax.optimization_barrier((half, every, every_far))
    spread = lax.all_to_all(half.reshape(COUNT, 9, 2, DEPTH), PEERS, 0, 0)
    table, g_up = pl.pallas_call(
        coarse_kernel,
        in_specs=[smem(), vmem(), far(), far(), far()],
        out_specs=[far(), vmem()],
        out_shape=[pltpu.HBM((9, DEPTH, WIDE), BF16), shape((WIDE, DEPTH), F32)],
        scratch_shapes=[
            pltpu.VMEM((COUNT * PACK, DEPTH), BF16),
            pltpu.VMEM((COUNT * PACK, DEPTH), BF16),
            pltpu.VMEM((9 * DEPTH, WIDE), BF16),
            pltpu.VMEM((9, DEPTH, WIDE), BF16),
            pltpu.VMEM(((GROW + 2) * GCOL, 3 * DEPTH), BF16),
            pltpu.VMEM((CELLS, DEPTH), BF16),
            pltpu.VMEM((CELLS, WIDE), BF16),
            pltpu.VMEM((CELLS + 2 * GCOL, WIDE), BF16),
            pltpu.SemaphoreType.DMA((6,)),
        ],
        name="coarse",
        compiler_params=grant(56),
    )(pos, w_up, held(every), held(every_far), held(w_eff))
    spread, table = lax.optimization_barrier((spread, table))
    total = pl.pallas_call(
        fold_kernel,
        in_specs=[vmem()],
        out_specs=vmem(),
        out_shape=pltpu.VMEM((2 * HALF, DEPTH), BF16),
        name="fold",
        compiler_params=grant(8),
    )(spread.reshape(HALF, DEPTH))
    total, table, merged, dact = lax.optimization_barrier((total, table, merged, dact))
    whole = lax.all_to_all(total.reshape(2 * COUNT, 9, 2, DEPTH), EVERYONE, 0, 0)
    g_bot, block_out, field_grad, g_down = pl.pallas_call(
        tail_kernel,
        in_specs=[vmem()] + [far()] * 6,
        out_specs=[far()] * 3 + [vmem()],
        out_shape=[
            pltpu.HBM((9, WIDE, WIDE), F32),
            pltpu.HBM((ROWS, COLS, DEPTH), BF16),
            pltpu.HBM((ROWS, COLS, DEPTH), BF16),
            shape((DEPTH, WIDE), F32),
        ],
        scratch_shapes=[
            pltpu.VMEM((9, DEPTH, WIDE), BF16),
            pltpu.VMEM((RIM, DEPTH), BF16),
            pltpu.VMEM((RIM, DEPTH), BF16),
            pltpu.VMEM((3, 3 * DEPTH, DEPTH), BF16),
            pltpu.VMEM((9, DEPTH, DEPTH), BF16),
            pltpu.VMEM((9, WIDE, WIDE), BF16),
            pltpu.VMEM((9, WIDE, WIDE), F32),
            pltpu.VMEM((RIM, 3 * DEPTH), BF16),
            pltpu.VMEM((RIM, 3 * DEPTH), BF16),
            pltpu.VMEM((ROWS, STRIDE, DEPTH), BF16),
            pltpu.VMEM((ROWS, STRIDE, DEPTH), BF16),
            pltpu.SemaphoreType.DMA((25,)),
        ],
        name="tail",
        compiler_params=grant(56),
    )(
        w_down,
        *(
            held(x)
            for x in (
                table, merged, dact, w_dec_f,
                w_enc.reshape(9, DEPTH, DEPTH), w_bot.reshape(9, WIDE, WIDE),
            )
        ),
    )
    whole, g_bot, block_out = lax.optimization_barrier((whole, g_bot, block_out))
    g_dec, g_enc = pl.pallas_call(
        finish_kernel,
        in_specs=[vmem()],
        out_specs=[vmem()] * 2,
        out_shape=[shape((HALF, DEPTH), F32)] * 2,
        name="finish",
        compiler_params=grant(6),
    )(whole.reshape(2 * HALF, DEPTH))
    g_dec = g_dec.reshape(3, 3, DEPTH, DEPTH)
    g_enc = g_enc.reshape(3, 3, DEPTH, DEPTH)
    return (block_out, field_grad, g_enc, g_down, g_bot.reshape(3, 3, WIDE, WIDE), g_up, g_dec)


def solution(mesh):
    split = Mesh(mesh.devices.reshape(NLAT, NLON // 2, 2), ("lat",) + LON)
    tile = P("lat", LON, None)
    return jax.shard_map(
        body,
        mesh=split,
        in_specs=(tile, P(), P(), P(), P(), P(), tile),
        out_specs=(tile, tile, P(), P(), P(), P(), P()),
        check_vma=False,
    )
```

```python
import jax
import jax.numpy as jnp
from jax import lax
from jax.experimental import pallas as pl
from jax.experimental.pallas import tpu as pltpu
from jax.sharding import Mesh
from jax.sharding import PartitionSpec as P

POOL = 8
LON = ("pair", "core")
PEERS = ("lat", "pair")
EVERYONE = ("lat", "pair", "core")
ROWS, COLS, DEPTH = 16, 48, 128
WIDE = 512
STRIDE = 64
EXT = 21 * STRIDE
RIM = 19 * STRIDE
OWN = ROWS * STRIDE
CROW, CCOL = ROWS // POOL, COLS // POOL
NLAT, NLON = 8, 16
COUNT = NLAT * NLON // 2
HALF = COUNT * 18
GROW, GCOL = NLAT * CROW, NLON * CCOL
CELLS = GROW * GCOL
PACK = 2 * CROW * CCOL
WIN = 16
F32 = jnp.float32
BF16 = jnp.bfloat16


def mm(left, right, contract=((1,), (0,))):
    return lax.dot_general(left, right, (contract, ((), ())), preferred_element_type=F32)


def side_by_side(flat):
    wide = flat.astype(F32)
    low = pltpu.roll(wide, 1, 0).astype(BF16)
    high = pltpu.roll(wide, flat.shape[0] - 1, 0).astype(BF16)
    return jnp.concatenate([low, flat.astype(BF16), high], axis=1)


def split_two(value):
    high = value.astype(BF16)
    return high, (value - high.astype(F32)).astype(BF16)


def rim_position(shape, dim):
    spot = lax.broadcasted_iota(jnp.int32, shape, dim)
    slot = spot & (STRIDE - 1)
    line = spot >> 6
    left = slot == STRIDE - 1
    row = jnp.where(left, line - 1, line - 2)
    col = jnp.where(left, -1, slot)
    return row, col


def row_live(row, lat):
    return jnp.logical_and(
        jnp.logical_or(row >= 0, lat > 0), jnp.logical_or(row < ROWS, lat < NLAT - 1)
    )


def mirrored(kernel, tap):
    base = 3 * (2 - tap)
    return jnp.concatenate([kernel[base + 2], kernel[base + 1], kernel[base]], axis=1)


def first_kernel(
    pos, got_inner, got_outer, strip, fine, grad, w_enc_far, w_dec_far,
    pack_out, hid_out, slope_out, dm_out, field_out,
    pack, field, grad_field, fine_cat, grad_cat, hid_here, slope_here, dm_here, w_enc, w_dec, sems,
):
    lat = pos[0]
    even = lat % 2 == 0
    fetches = [
        pltpu.make_async_copy(a, b, sems.at[5 + k])
        for k, (a, b) in enumerate(
            (
                (fine, field.at[3:19, 0:COLS, :]),
                (grad, grad_field.at[3:19, 0:COLS, :]),
                (w_enc_far, w_enc),
                (w_dec_far, w_dec),
            )
        )
    ]
    for fetch in fetches:
        fetch.start()
    sources = (field, hid_here, slope_here, dm_here, pack)
    targets = (field_out, hid_out, slope_out, dm_out, pack_out)
    copies = [
        pltpu.make_async_copy(a, b, sems.at[k]) for k, (a, b) in enumerate(zip(sources, targets))
    ]
    for part, (space, cat) in enumerate(((field, fine_cat), (grad_field, grad_cat))):
        lanes = slice(part * DEPTH, (part + 1) * DEPTH)
        space[0:1, 0:COLS, :] = jnp.zeros((1, COLS, DEPTH), BF16)
        inner = got_inner[2 * part : 2 * part + 2]
        outer = got_outer[2 * part : 2 * part + 2]
        space[1:3, 0:COLS, :] = jnp.where(even, outer, inner)
        space[19:21, 0:COLS, :] = jnp.where(even, inner, outer)
        space[:, COLS:STRIDE, :] = strip[:, :, lanes]
        fetches[part].wait()
        if part == 0:
            copies[0].start()
        cat[...] = side_by_side(space[...].reshape(EXT, DEPTH))
    act = jnp.zeros((RIM, DEPTH), F32)
    fetches[2].wait()
    for tap in range(3):
        act = act + mm(fine_cat[tap * STRIDE : tap * STRIDE + RIM, :], w_enc[tap])
    row, _ = rim_position((RIM, 1), 0)
    live = row_live(row, lat)
    sig = jax.nn.sigmoid(act)
    hid = jnp.where(live, act * sig, 0.0).astype(BF16)
    hid_here[...] = hid
    copies[1].start()
    slope_here[...] = jnp.where(live, sig * (1.0 + act * (1.0 - sig)), 0.0)
    copies[2].start()
    dm = jnp.zeros((RIM, DEPTH), F32)
    fetches[3].wait()
    for tap in range(3):
        dm = dm + mm(
            grad_cat[tap * STRIDE : tap * STRIDE + RIM, :], mirrored(w_dec, tap), ((1,), (1,))
        )
    dm_here[...] = dm
    copies[3].start()
    half = PACK // 2
    prow, pcol = rim_position((PACK, RIM), 1)
    which = lax.broadcasted_iota(jnp.int32, (PACK, RIM), 0)
    inside = (prow >= 0) & (prow < ROWS) & (pcol >= 0) & (pcol < COLS)
    cell = jnp.where(inside, (prow >> 3) * CCOL + (pcol >> 3), -1)
    take_hid = (cell == which).astype(F32).astype(BF16)
    take_dm = (inside & (cell + half == which)).astype(F32).astype(BF16)
    dm_high, dm_low = split_two(dm)
    packed = mm(take_hid, hid) * (1.0 / (POOL * POOL)) + (mm(take_dm, dm_high) + mm(take_dm, dm_low))
    packed = packed.astype(BF16)
    for peer in range(COUNT):
        pack[peer] = packed
    copies[4].start()
    for copy in copies:
        copy.wait()


def weight_kernel(w_down, w_bot_far, out_far, w_bot, out, sems):
    fetches = [pltpu.make_async_copy(w_bot_far.at[k], w_bot.at[k], sems.at[k]) for k in range(9)]
    stores = [pltpu.make_async_copy(out.at[k], out_far.at[k], sems.at[9 + k]) for k in range(9)]
    for fetch in fetches:
        fetch.start()
    for k in range(9):
        fetches[k].wait()
        out[k] = mm(w_down[...], w_bot[k]).astype(BF16)
        stores[k].start()
    for store in stores:
        store.wait()


def third(value):
    return (value * 43) >> 8


def source_of(row, col, shift, core, first, lats):
    inside = (row >= 0) & (row < GROW)
    col = jnp.where(col < 0, col + GCOL, col)
    col = jnp.where(col >= GCOL, col - GCOL, col)
    group = third(col)
    place = ((row >> 1) - first) * (NLON // 2) + (group >> 1)
    half = jnp.where((group & 1) == core, 0, lats * (NLON // 2) * PACK)
    return jnp.where(
        inside, half + place * PACK + shift + (row & 1) * CCOL + (col - group * CCOL), -1
    )


def second_kernel(
    pos, every, every_far, w_up, w_eff_far, hid_far, slope_far, dm_far, field_far, grad_far,
    parts_out, merged_out, dact_out,
    parts, w_eff, hid, slope, dm, field, own_grad, fine_cat, merged_cat, merged_here, dact_here, sems,
):
    lat, lon, core = pos[0], pos[1], pos[2]
    fetches = [
        pltpu.make_async_copy(a, b, sems.at[k])
        for k, (a, b) in enumerate(
            (
                (w_eff_far, w_eff),
                (field_far, field),
                (hid_far, hid),
                (dm_far, dm),
                (slope_far, slope),
                (grad_far, own_grad.at[:, 0:COLS, :]),
            )
        )
    ]
    stores = [
        pltpu.make_async_copy(merged_here, merged_out, sems.at[6]),
        pltpu.make_async_copy(dact_here, dact_out, sems.at[7]),
        pltpu.make_async_copy(parts.at[0:HALF, :], parts_out.at[0:HALF, :], sems.at[8]),
        pltpu.make_async_copy(parts.at[HALF:, :], parts_out.at[HALF:, :], sems.at[9]),
    ]
    for fetch in fetches:
        fetch.start()
    own_grad[:, COLS:, :] = jnp.zeros((ROWS, STRIDE - COLS, DEPTH), BF16)
    lats = 5
    first = jnp.clip(lat - 2, 0, NLAT - lats)
    spot = lax.broadcasted_iota(jnp.int32, (8 * WIN, 1), 0)
    line, slot = spot >> 4, spot & (WIN - 1)
    src = source_of(CROW * lat + line - 3, CCOL * lon + slot - 3, 0, core, first, lats)
    src = jnp.where(slot < CCOL + 6, src, -1)
    spot = lax.broadcasted_iota(jnp.int32, (6 * WIN, 1), 0)
    line, slot = spot >> 4, spot & (WIN - 1)
    dsrc = source_of(
        CROW * lat + line - 2, CCOL * lon + slot - 2, CROW * CCOL, core, first, lats
    )
    dsrc = jnp.where(slot < CCOL + 4, dsrc, -1)
    strip = NLON // 2 * PACK
    begin = pl.multiple_of(first * strip, strip)
    reach = lats * strip
    near = jnp.concatenate(
        [every[pl.ds(begin, reach), :], every_far[pl.ds(begin, reach), :]], axis=0
    )
    spots = lax.broadcasted_iota(jnp.int32, (8 * WIN, 2 * reach), 1)
    pooled = mm((spots == src).astype(F32).astype(BF16), near)
    spots = lax.broadcasted_iota(jnp.int32, (6 * WIN, 2 * reach), 1)
    dlift = mm((spots == dsrc).astype(F32).astype(BF16), near).astype(BF16)
    shifted = [pooled.astype(BF16)] + [
        pltpu.roll(pooled, 8 * WIN - step, 0).astype(BF16) for step in (1, 2)
    ]
    pooled_cat = jnp.concatenate(shifted, axis=1)
    zpre = jnp.zeros((6 * WIN, WIDE), F32)
    fetches[0].wait()
    for tap in range(3):
        zpre = zpre + mm(
            pooled_cat[tap * WIN : tap * WIN + 6 * WIN], w_eff[tap * 384 : tap * 384 + 384, :]
        )
    sig = jax.nn.sigmoid(zpre)
    zact = (zpre * sig).astype(BF16)
    dz = mm(dlift, w_up[...], ((1,), (1,))) * (sig * (1.0 + zpre * (1.0 - sig)))
    dz = dz.astype(BF16)
    lifted = mm(zact, w_up[...])
    taps = mm(dz, w_eff[...], ((1,), (1,)))
    dpool = jnp.zeros((6 * WIN, DEPTH), F32)
    for tap_a in range(3):
        for tap_b in range(3):
            spot = ((2 - tap_a) * 3 + (2 - tap_b)) * DEPTH
            turn = ((1 - tap_a) * WIN + (1 - tap_b)) % (6 * WIN)
            part = taps[:, spot : spot + DEPTH]
            dpool = dpool + (part if turn == 0 else pltpu.roll(part, turn, 0))
    dpool = dpool * (1.0 / (POOL * POOL))
    lift_high, lift_low = split_two(lifted)
    pool_high, pool_low = split_two(dpool)
    tail = jnp.zeros((2 * WIN, 2 * DEPTH), BF16)
    table = jnp.concatenate(
        [
            jnp.concatenate([lift_high, pool_high], axis=1),
            tail,
            jnp.concatenate([lift_low, pool_low], axis=1),
            tail,
        ],
        axis=0,
    )
    row, col = rim_position((RIM, 1), 0)
    home = (((row + POOL) >> 3) + 1) * WIN + ((col + POOL) >> 3) + 1
    home = jnp.where(col <= COLS, home, -1)
    cells = lax.broadcasted_iota(jnp.int32, (RIM, 256), 1) & 127
    spread = mm((cells == home).astype(F32).astype(BF16), table)
    live = row_live(row, lat)
    for fetch in fetches[1:]:
        fetch.wait()
    merged = jnp.where(live, hid[...].astype(F32) + spread[:, :DEPTH], 0.0)
    dact = (dm[...] + spread[:, DEPTH:]) * slope[...]
    merged_here[...] = merged.astype(BF16)
    stores[0].start()
    dact_here[...] = dact.astype(BF16)
    stores[1].start()
    merged_cat[...] = side_by_side(merged.astype(BF16))
    fine_cat[...] = side_by_side(field[...].reshape(EXT, DEPTH))
    slot = lax.broadcasted_iota(jnp.int32, (OWN, 1), 0) & (STRIDE - 1)
    center = dact_here[2 * STRIDE : 2 * STRIDE + OWN, :]
    own_dact = jnp.where(slot < COLS, center, jnp.zeros_like(center))
    center_grad = own_grad[...].reshape(OWN, DEPTH)
    for tap in range(3):
        start = (tap + 1) * STRIDE
        parts[tap * 384 : tap * 384 + 384, :] = mm(
            merged_cat[start : start + OWN, :], center_grad, ((0,), (0,))
        ).astype(BF16)
    stores[2].start()
    for tap in range(3):
        start = (tap + 2) * STRIDE
        parts[HALF + tap * 384 : HALF + tap * 384 + 384, :] = mm(
            fine_cat[start : start + OWN, :], own_dact, ((0,), (0,))
        ).astype(BF16)
    stores[3].start()
    for store in stores:
        store.wait()


def coarse_kernel(
    pos, w_up, every_out, every_far_out, w_eff_out, table_out, g_up,
    every, every_far, w_eff, table, pooled_cat, dlift, zact, dz, sems,
):
    fetches = [
        pltpu.make_async_copy(a, b, sems.at[k])
        for k, (a, b) in enumerate(
            ((every_out, every), (every_far_out, every_far), (w_eff_out, w_eff))
        )
    ]
    stores = [
        pltpu.make_async_copy(
            table.at[3 * k : 3 * k + 3], table_out.at[3 * k : 3 * k + 3], sems.at[3 + k]
        )
        for k in range(3)
    ]
    for fetch in fetches:
        fetch.start()
    line = 2 * GCOL
    core = pos[2]
    strip = NLON // 2 * PACK
    spot = lax.broadcasted_iota(jnp.int32, (4 * line, 1), 0)
    kind = (spot >= line).astype(jnp.int32) + (spot >= 2 * line).astype(jnp.int32)
    kind = kind + (spot >= 3 * line).astype(jnp.int32)
    within = spot - kind * line
    row = (within >= GCOL).astype(jnp.int32)
    col = within - row * GCOL
    col = jnp.where(kind < 3, col + kind - 1, col)
    shift = jnp.where(kind < 3, 0, CROW * CCOL)
    src = source_of(row, col, shift, core, 0, 1)
    spots = lax.broadcasted_iota(jnp.int32, (4 * line, 2 * strip), 1)
    order = (spots == src).astype(F32).astype(BF16)
    edge = jnp.zeros((GCOL, 3 * DEPTH), BF16)
    pooled_cat[0:GCOL, :] = edge
    pooled_cat[(GROW + 1) * GCOL :, :] = edge
    fetches[0].wait()
    fetches[1].wait()
    for pair in range(NLAT // 2):
        both = jnp.concatenate(
            [
                jnp.concatenate(
                    [part[(2 * pair + k) * strip : (2 * pair + k + 1) * strip, :] for k in (0, 1)],
                    axis=1,
                )
                for part in (every, every_far)
            ],
            axis=0,
        )
        moved = mm(order, both).astype(BF16)
        for k in (0, 1):
            lat = 2 * pair + k
            lanes = slice(k * DEPTH, (k + 1) * DEPTH)
            at = GCOL + lat * line
            for b in range(3):
                pooled_cat[at : at + line, b * DEPTH : (b + 1) * DEPTH] = moved[
                    b * line : (b + 1) * line, lanes
                ]
            dlift[lat * line : (lat + 1) * line, :] = moved[3 * line :, lanes]
    fetches[2].wait()
    rows = 384
    for part in range(CELLS // rows):
        base = part * rows
        spread = jnp.concatenate(
            [pooled_cat[base + tap * GCOL : base + tap * GCOL + rows, :] for tap in range(3)], axis=1
        )
        zpre = mm(spread, w_eff[...])
        sig = jax.nn.sigmoid(zpre)
        zact[base : base + rows, :] = (zpre * sig).astype(BF16)
        up = mm(dlift[base : base + rows, :], w_up[...], ((1,), (1,)))
        dz[GCOL + base : GCOL + base + rows, :] = (up * (sig * (1.0 + zpre * (1.0 - sig)))).astype(BF16)
    blank = jnp.zeros((GCOL, WIDE), BF16)
    dz[0:GCOL, :] = blank
    dz[GCOL + CELLS :, :] = blank
    lying = pooled_cat[GCOL : GCOL + CELLS, :].T
    for tap in range(3):
        at = (2 - tap) * GCOL
        corr = mm(lying, dz[at : at + CELLS, :]).astype(BF16)
        table[3 * tap : 3 * tap + 3] = corr.reshape(3, DEPTH, WIDE)
        stores[tap].start()
    g_up[...] = mm(dlift[...].T, zact[...]).T
    for store in stores:
        store.wait()


def remainder(value):
    return value - 18 * ((value * 3641) >> 16)


def fold_kernel(spread, out):
    full = 2 * HALF
    slot = remainder(lax.broadcasted_iota(jnp.int32, (32, full), 1))
    pick = slot == lax.broadcasted_iota(jnp.int32, (32, full), 0)
    total = mm(pick.astype(F32).astype(BF16), spread[...]).astype(BF16)
    slot = remainder(lax.broadcasted_iota(jnp.int32, (full, 1), 0))
    copy = lax.broadcasted_iota(jnp.int32, (full, 32), 1) == slot
    out[...] = mm(copy.astype(F32).astype(BF16), total).astype(BF16)


def finish_kernel(whole, g_dec, g_enc):
    g_dec[...] = whole[:HALF].astype(F32)
    g_enc[...] = whole[HALF:].astype(F32)


def tail_kernel(
    w_down, table_far, merged_far, dact_far, w_dec_far, w_enc_far, w_bot_far,
    g_bot_far, block_far, back_far, g_down,
    table, merged, dact, w_dec, w_enc, w_bot, g_bot, merged_cat, dact_cat, block, back, sems,
):
    fetches = [
        pltpu.make_async_copy(a, b, sems.at[18 + k])
        for k, (a, b) in enumerate(
            (
                (table_far, table),
                (merged_far, merged),
                (dact_far, dact),
                (w_dec_far, w_dec),
                (w_enc_far, w_enc),
            )
        )
    ]
    loads = [pltpu.make_async_copy(w_bot_far.at[k], w_bot.at[k], sems.at[k]) for k in range(9)]
    stores = [pltpu.make_async_copy(g_bot.at[k], g_bot_far.at[k], sems.at[9 + k]) for k in range(9)]
    stores.append(pltpu.make_async_copy(block.at[:, 0:COLS, :], block_far, sems.at[23]))
    stores.append(pltpu.make_async_copy(back.at[:, 0:COLS, :], back_far, sems.at[24]))
    for fetch in fetches:
        fetch.start()
    for load in loads:
        load.start()
    fetches[0].wait()
    for k in range(9):
        g_bot[k] = mm(w_down[...], table[k], ((0,), (0,)))
        stores[k].start()
    for fetch in fetches[1:]:
        fetch.wait()
    merged_cat[...] = side_by_side(merged[...])
    dact_cat[...] = side_by_side(dact[...])
    fore = jnp.zeros((OWN, DEPTH), F32)
    aft = jnp.zeros((OWN, DEPTH), F32)
    for tap in range(3):
        start = (tap + 1) * STRIDE
        fore = fore + mm(merged_cat[start : start + OWN, :], w_dec[tap])
        aft = aft + mm(dact_cat[start : start + OWN, :], mirrored(w_enc, tap), ((1,), (1,)))
    block[...] = fore.astype(BF16).reshape(ROWS, STRIDE, DEPTH)
    stores[9].start()
    back[...] = aft.astype(BF16).reshape(ROWS, STRIDE, DEPTH)
    stores[10].start()
    total = jnp.zeros((DEPTH, WIDE), F32)
    for k in range(9):
        loads[k].wait()
        total = total + mm(table[k], w_bot[k], ((1,), (1,)))
    g_down[...] = total
    for store in stores:
        store.wait()


def vmem():
    return pl.BlockSpec(memory_space=pltpu.VMEM)


def far():
    return pl.BlockSpec(memory_space=pltpu.HBM)


def smem():
    return pl.BlockSpec(memory_space=pltpu.SMEM)


def shape(dims, kind):
    return jax.ShapeDtypeStruct(dims, kind)


def held(value):
    return pltpu.with_memory_space_constraint(value, pltpu.HBM)


def grant(mib):
    return pltpu.CompilerParams(vmem_limit_bytes=mib * 1024 * 1024)


def body(fine, w_enc, w_down, w_bot, w_up, w_dec, grad):
    pos = jnp.stack([lax.axis_index("lat"), lax.axis_index(LON), lax.axis_index("core")])
    pos = pos.astype(jnp.int32)
    swap = [(0, 1), (1, 0)]
    inner = [(i, i ^ 1) for i in range(NLAT)]
    outer = [(i, ((i + 1) ^ 1) - 1) for i in range(1, NLAT - 1)]
    even = lax.axis_index("lat") % 2 == 0
    right = [(i, (i + 1) % NLON) for i in range(NLON)]
    left = [(t, s) for s, t in right]
    under = jnp.concatenate([fine[-2:], grad[-2:]], axis=0)
    over = jnp.concatenate([fine[:2], grad[:2]], axis=0)
    got_inner = lax.ppermute(jnp.where(even, under, over), "lat", inner)
    got_outer = lax.ppermute(jnp.where(even, over, under), "lat", outer)
    top = jnp.where(even, got_outer, got_inner)
    bot = jnp.where(even, got_inner, got_outer)

    def edge(cols):
        return jnp.concatenate(
            [
                jnp.concatenate([top[at : at + 2, cols], tile[:, cols], bot[at : at + 2, cols]], axis=0)
                for at, tile in ((0, fine), (2, grad))
            ],
            axis=2,
        )

    first = edge(slice(0, 2))
    last = edge(slice(COLS - 2, COLS))
    high = lax.ppermute(first, LON, left)
    low = lax.ppermute(last, LON, right)
    strip = jnp.concatenate(
        [
            jnp.pad(high, ((1, 0), (0, 0), (0, 0))),
            jnp.zeros((21, 12, 2 * DEPTH), BF16),
            jnp.pad(low, ((0, 1), (0, 0), (0, 0))),
        ],
        axis=1,
    )
    w_enc_f = w_enc.reshape(3, 3 * DEPTH, DEPTH)
    w_dec_f = w_dec.reshape(3, 3 * DEPTH, DEPTH)
    pack, hid, slope, dm, field = pl.pallas_call(
        first_kernel,
        in_specs=[smem()] + [vmem()] * 3 + [far()] * 4,
        out_specs=[far()] * 5,
        out_shape=[
            pltpu.HBM((COUNT, PACK, DEPTH), BF16),
            pltpu.HBM((RIM, DEPTH), BF16),
            pltpu.HBM((RIM, DEPTH), F32),
            pltpu.HBM((RIM, DEPTH), F32),
            pltpu.HBM((21, STRIDE, DEPTH), BF16),
        ],
        scratch_shapes=[
            pltpu.VMEM((COUNT, PACK, DEPTH), BF16),
            pltpu.VMEM((21, STRIDE, DEPTH), BF16),
            pltpu.VMEM((21, STRIDE, DEPTH), BF16),
            pltpu.VMEM((EXT, 3 * DEPTH), BF16),
            pltpu.VMEM((EXT, 3 * DEPTH), BF16),
            pltpu.VMEM((RIM, DEPTH), BF16),
            pltpu.VMEM((RIM, DEPTH), F32),
            pltpu.VMEM((RIM, DEPTH), F32),
            pltpu.VMEM((3, 3 * DEPTH, DEPTH), BF16),
            pltpu.VMEM((9, DEPTH, DEPTH), BF16),
            pltpu.SemaphoreType.DMA((9,)),
        ],
        name="first",
        compiler_params=grant(30),
    )(
        pos, got_inner, got_outer, strip,
        *(held(x) for x in (fine, grad, w_enc_f, w_dec.reshape(9, DEPTH, DEPTH))),
    )
    pack, early = lax.optimization_barrier((pack, w_down))
    every = lax.all_to_all(pack, PEERS, 0, 0).reshape(COUNT * PACK, DEPTH)
    w_eff = pl.pallas_call(
        weight_kernel,
        in_specs=[vmem(), far()],
        out_specs=far(),
        out_shape=pltpu.HBM((9, DEPTH, WIDE), BF16),
        scratch_shapes=[
            pltpu.VMEM((9, WIDE, WIDE), BF16),
            pltpu.VMEM((9, DEPTH, WIDE), BF16),
            pltpu.SemaphoreType.DMA((18,)),
        ],
        name="weights",
        compiler_params=grant(56),
    )(early, held(w_bot.reshape(9, WIDE, WIDE))).reshape(9 * DEPTH, WIDE)
    every, w_eff = lax.optimization_barrier((every, w_eff))
    every_far = lax.ppermute(every, "core", swap)
    parts, merged, dact = pl.pallas_call(
        second_kernel,
        in_specs=[smem(), vmem(), vmem(), vmem()] + [far()] * 6,
        out_specs=[far()] * 3,
        out_shape=[
            pltpu.HBM((2 * HALF, DEPTH), BF16),
            pltpu.HBM((RIM, DEPTH), BF16),
            pltpu.HBM((RIM, DEPTH), BF16),
        ],
        scratch_shapes=[
            pltpu.VMEM((2 * HALF, DEPTH), BF16),
            pltpu.VMEM((9 * DEPTH, WIDE), BF16),
            pltpu.VMEM((RIM, DEPTH), BF16),
            pltpu.VMEM((RIM, DEPTH), F32),
            pltpu.VMEM((RIM, DEPTH), F32),
            pltpu.VMEM((21, STRIDE, DEPTH), BF16),
            pltpu.VMEM((ROWS, STRIDE, DEPTH), BF16),
            pltpu.VMEM((EXT, 3 * DEPTH), BF16),
            pltpu.VMEM((RIM, 3 * DEPTH), BF16),
            pltpu.VMEM((RIM, DEPTH), BF16),
            pltpu.VMEM((RIM, DEPTH), BF16),
            pltpu.SemaphoreType.DMA((10,)),
        ],
        name="second",
        compiler_params=grant(30),
    )(pos, every, every_far, w_up, *(held(x) for x in (w_eff, hid, slope, dm, field, grad)))
    parts, every, every_far, merged, dact = lax.optimization_barrier(
        (parts, every, every_far, merged, dact)
    )
    spread = lax.all_to_all(parts.reshape(2 * COUNT, 9, 2, DEPTH), EVERYONE, 0, 0)
    table, g_up = pl.pallas_call(
        coarse_kernel,
        in_specs=[smem(), vmem(), far(), far(), far()],
        out_specs=[far(), vmem()],
        out_shape=[pltpu.HBM((9, DEPTH, WIDE), BF16), shape((WIDE, DEPTH), F32)],
        scratch_shapes=[
            pltpu.VMEM((COUNT * PACK, DEPTH), BF16),
            pltpu.VMEM((COUNT * PACK, DEPTH), BF16),
            pltpu.VMEM((9 * DEPTH, WIDE), BF16),
            pltpu.VMEM((9, DEPTH, WIDE), BF16),
            pltpu.VMEM(((GROW + 2) * GCOL, 3 * DEPTH), BF16),
            pltpu.VMEM((CELLS, DEPTH), BF16),
            pltpu.VMEM((CELLS, WIDE), BF16),
            pltpu.VMEM((CELLS + 2 * GCOL, WIDE), BF16),
            pltpu.SemaphoreType.DMA((6,)),
        ],
        name="coarse",
        compiler_params=grant(56),
    )(pos, w_up, held(every), held(every_far), held(w_eff))
    spread, table = lax.optimization_barrier((spread, table))
    total = pl.pallas_call(
        fold_kernel,
        in_specs=[vmem()],
        out_specs=vmem(),
        out_shape=pltpu.VMEM((2 * HALF, DEPTH), BF16),
        name="fold",
        compiler_params=grant(8),
    )(spread.reshape(2 * HALF, DEPTH))
    total, table, merged, dact = lax.optimization_barrier((total, table, merged, dact))
    whole = lax.all_to_all(total.reshape(2 * COUNT, 9, 2, DEPTH), EVERYONE, 0, 0)
    g_bot, block_out, field_grad, g_down = pl.pallas_call(
        tail_kernel,
        in_specs=[vmem()] + [far()] * 6,
        out_specs=[far()] * 3 + [vmem()],
        out_shape=[
            pltpu.HBM((9, WIDE, WIDE), F32),
            pltpu.HBM((ROWS, COLS, DEPTH), BF16),
            pltpu.HBM((ROWS, COLS, DEPTH), BF16),
            shape((DEPTH, WIDE), F32),
        ],
        scratch_shapes=[
            pltpu.VMEM((9, DEPTH, WIDE), BF16),
            pltpu.VMEM((RIM, DEPTH), BF16),
            pltpu.VMEM((RIM, DEPTH), BF16),
            pltpu.VMEM((3, 3 * DEPTH, DEPTH), BF16),
            pltpu.VMEM((9, DEPTH, DEPTH), BF16),
            pltpu.VMEM((9, WIDE, WIDE), BF16),
            pltpu.VMEM((9, WIDE, WIDE), F32),
            pltpu.VMEM((RIM, 3 * DEPTH), BF16),
            pltpu.VMEM((RIM, 3 * DEPTH), BF16),
            pltpu.VMEM((ROWS, STRIDE, DEPTH), BF16),
            pltpu.VMEM((ROWS, STRIDE, DEPTH), BF16),
            pltpu.SemaphoreType.DMA((25,)),
        ],
        name="tail",
        compiler_params=grant(56),
    )(
        w_down,
        *(
            held(x)
            for x in (
                table, merged, dact, w_dec_f,
                w_enc.reshape(9, DEPTH, DEPTH), w_bot.reshape(9, WIDE, WIDE),
            )
        ),
    )
    whole, g_bot, block_out = lax.optimization_barrier((whole, g_bot, block_out))
    g_dec, g_enc = pl.pallas_call(
        finish_kernel,
        in_specs=[vmem()],
        out_specs=[vmem()] * 2,
        out_shape=[shape((HALF, DEPTH), F32)] * 2,
        name="finish",
        compiler_params=grant(6),
    )(whole.reshape(2 * HALF, DEPTH))
    g_dec = g_dec.reshape(3, 3, DEPTH, DEPTH)
    g_enc = g_enc.reshape(3, 3, DEPTH, DEPTH)
    return (block_out, field_grad, g_enc, g_down, g_bot.reshape(3, 3, WIDE, WIDE), g_up, g_dec)


def solution(mesh):
    split = Mesh(mesh.devices.reshape(NLAT, NLON // 2, 2), ("lat",) + LON)
    tile = P("lat", LON, None)
    return jax.shard_map(
        body,
        mesh=split,
        in_specs=(tile, P(), P(), P(), P(), P(), tile),
        out_specs=(tile, tile, P(), P(), P(), P(), P()),
        check_vma=False,
    )
```
